256 devices in a mesh: gx: 4 (over y), gy: 8 (over z), gz: 8 (over x, core).
Axes of the slice: x: 4, y: 4, z: 8, core: 2. Of those that a mesh axis runs over, the one named last changes fastest.
Arguments:
- descriptors: float32 [64, 2097152], P(None, ('gx', 'gy', 'gz')), may hold values from -6 to 6
- types: int32 [2097152], P(('gx', 'gy', 'gz')), may hold values from 0 to 2
- offsets: float32 [3, 2097152], P(None, ('gx', 'gy', 'gz')), may hold values from 0 to 1
- stencil_base: int32 [3, 2097152], P(None, ('gx', 'gy', 'gz')), may hold values from 0 to 47, as said below
- w_first: float32 [3, 25, 64], replicated, may hold values from -0.75 to 0.75
- w_second: float32 [3, 25, 25], replicated, may hold values from -1.25 to 1.25
- w_out: float32 [3, 25], replicated, may hold values from -1.25 to 1.25
- hardness: float32 [3], replicated, may hold values from 0.5 to 3
- sr_first: float32 [3, 25, 64], replicated, may hold values from -0.75 to 0.75
- sr_charge: float32 [3, 25], replicated, may hold values from -6 to 6
- sr_out: float32 [3, 25], replicated, may hold values from -1.25 to 1.25
Outputs:
- charges: float32 [2097152], P(('gx', 'gy', 'gz'))
- forces: float32 [3, 2097152], P(None, ('gx', 'gy', 'gz'))
- short_energy: float32 [2097152], P(('gx', 'gy', 'gz'))
The draws below stay inside these ranges and needn't reach their ends.
Inputs may be any that keep to these rules, and one draw needn't show every extreme that they name: stencil_base[d, a] is a cell of the atom's brick: below 48, 24 and 24 for d = 0, 1, 2.
All inputs are finite; a program needn't handle non-finite values.
Results may differ from the reference program's by a relative error of at most 0.0003.
Values sent between devices are 32-bit elements; how exact they have to be, the bound alone decides.
A program may use at most 320 MiB of HBM per device.

```python
import math
import jax
import jax.numpy as jnp
from jax import lax

M = 192
FEAT = 64
HID = 25
ELEMENTS = 3
ITERS = 2
A_DEV = 8192
BX = 48
BY = 24
BZ = 24
ATOMS = 2097152
N_GY = 8
N_GZ = 8


def draw_stencil_base(key, part):
    limits = jnp.array([[BX], [BY], [BZ]], dtype=jnp.int32)
    return jax.random.randint(key, (3, ATOMS), 0, limits, dtype=jnp.int32)


def plant(entries, rng, low, top_value):
    shape = entries.shape
    index_at = [jax.random.randint(jax.random.fold_in(rng, axis), (), 0, shape[axis]) for axis in range(len(shape))]
    entries = entries.at[tuple(index_at)].set(low)
    longest = shape.index(max(shape))
    index_at[longest] = (index_at[longest] + 1) % shape[longest]
    return entries.at[tuple(index_at)].set(top_value)


def steps_of(key, extent, split, least, top_value):
    def one(axis_at, parts):
        steps = jax.random.uniform(jax.random.fold_in(jax.random.fold_in(key, 6), axis_at), (parts,), jnp.float32, least / len(split), top_value / len(split))
        return jnp.repeat(jnp.exp(steps), extent[axis_at] // parts).reshape((-1,) + (1,) * (len(extent) - axis_at - 1))

    factor_of = one(*split[0])
    for cut in split[1:]:
        factor_of = factor_of * one(*cut)
    return factor_of


def bell_draw(stream_key, extent, deviation, limit, cuts=(), held_as=jnp.bfloat16):
    drawn = deviation * jax.random.normal(stream_key, extent, jnp.float32)
    if cuts:
        drawn = drawn * steps_of(stream_key, extent, cuts, -0.22, 0.18)
    return jnp.clip(drawn, -limit, limit).astype(held_as)


def setup_inputs(seed: int = 0) -> dict:
    streams_of = jax.random.split(jax.random.key(seed), 12)
    descriptors = bell_draw(streams_of[0], (FEAT, ATOMS), 1.0, 6.0, ((1, 256),), jnp.float32)
    types = plant(jax.random.randint(streams_of[1], (ATOMS,), 0, ELEMENTS), jax.random.fold_in(streams_of[1], 1), 0, ELEMENTS - 1).astype(jnp.int32)
    offsets = jnp.clip(1.0 * jax.random.uniform(streams_of[2], (3, ATOMS), jnp.float32) ** steps_of(streams_of[2], (3, ATOMS), ((1, 256),), -0.2, 0.2), 0.0, 1.0)
    stencil_base = draw_stencil_base(jax.random.fold_in(streams_of[11], 71), 0)
    w_first = bell_draw(streams_of[4], (ELEMENTS, HID, FEAT), FEAT ** -0.5, 0.75, (), jnp.float32)
    w_second = bell_draw(streams_of[5], (ELEMENTS, HID, HID), HID ** -0.5, 1.25, (), jnp.float32)
    w_out = bell_draw(streams_of[6], (ELEMENTS, HID), HID ** -0.5, 1.25, (), jnp.float32)
    hardness = jnp.clip(jnp.exp(jax.random.uniform(streams_of[7], (ELEMENTS,), jnp.float32, math.log(0.5), math.log(3.0))), 0.5, 3.0)
    sr_first = bell_draw(streams_of[8], (ELEMENTS, HID, FEAT), FEAT ** -0.5, 0.75, (), jnp.float32)
    sr_charge = bell_draw(streams_of[9], (ELEMENTS, HID), 2.0, 6.0, (), jnp.float32)
    sr_out = bell_draw(streams_of[10], (ELEMENTS, HID), HID ** -0.5, 1.25, (), jnp.float32)
    return dict(descriptors=descriptors, types=types, offsets=offsets, stencil_base=stencil_base, w_first=w_first, w_second=w_second, w_out=w_out, hardness=hardness, sr_first=sr_first, sr_charge=sr_charge, sr_out=sr_out)


smear = 0.75


def cardinal(order, offset):
    if order == 2:
        return jnp.maximum(1.0 - jnp.abs(offset - 1.0), 0.0)
    return (offset * cardinal(order - 1, offset) + (order - offset) * cardinal(order - 1, offset - 1.0)) / (order - 1)


def spline_tables(offsets):
    weights = jnp.stack([cardinal(5, offsets + 4.0 - point) for point in range(5)], axis=1)
    slopes = jnp.stack([cardinal(4, offsets + 4.0 - point) - cardinal(4, offsets + 3.0 - point) for point in range(5)], axis=1)
    return weights, slopes


def signed_freq(number, length):
    return jnp.where(2 * number >= length, number - length, number).astype(jnp.float32)


def green_values(first_freq, second_freq, third_freq, length):
    factor = 2.0 * math.pi / length
    wave = factor * factor * (first_freq * first_freq + second_freq * second_freq + third_freq * third_freq)
    safe = jnp.where(wave > 0, wave, 1.0)
    return jnp.where(wave > 0, 4.0 * math.pi * jnp.exp(-0.5 * smear * smear * wave) / safe, 0.0)


def element_net(first, second, final, descriptors, onehot):
    hidden = jnp.tanh(jnp.einsum('ehf,fa->eha', first, descriptors, precision=lax.Precision.HIGHEST))
    hidden = jnp.tanh(jnp.einsum('ehg,ega->eha', second, hidden, precision=lax.Precision.HIGHEST))
    output = jnp.einsum('eh,eha->ea', final, hidden, precision=lax.Precision.HIGHEST)
    return jnp.sum(onehot * output, axis=0)


def brick_cells(stencil_base):
    device = jnp.arange(ATOMS, dtype=jnp.int32) // A_DEV
    first_brick = device // (N_GY * N_GZ)
    second_brick = (device // N_GZ) % N_GY
    third_brick = device % N_GZ
    anchor = jnp.stack([first_brick * BX, second_brick * BY, third_brick * BZ]).astype(jnp.int32)
    return anchor + stencil_base - 2


def spread(values, cells, weights):
    grid = jnp.zeros((M * M * M,), jnp.float32)
    stencil = jnp.arange(5, dtype=jnp.int32)
    third_cells = (cells[2][None, :] + stencil[:, None]) % M
    for first in range(5):
        first_cells = (cells[0] + first) % M
        for second in range(5):
            second_cells = (cells[1] + second) % M
            index = (first_cells * M + second_cells)[None, :] * M + third_cells
            amount = (values * weights[0, first] * weights[1, second])[None, :] * weights[2]
            grid = grid.at[index.reshape(-1)].add(amount.reshape(-1))
    return grid.reshape(M, M, M)


def sample(field, cells, first_table, second_table, third_table):
    flat = field.reshape(-1)
    stencil = jnp.arange(5, dtype=jnp.int32)
    third_cells = (cells[2][None, :] + stencil[:, None]) % M
    result = jnp.zeros((cells.shape[1],), jnp.float32)
    for first in range(5):
        first_cells = (cells[0] + first) % M
        for second in range(5):
            second_cells = (cells[1] + second) % M
            index = (first_cells * M + second_cells)[None, :] * M + third_cells
            inner = jnp.sum(flat[index] * third_table, axis=0)
            result = result + first_table[first] * second_table[second] * inner
    return result


def poisson(density):
    freq = signed_freq(jnp.arange(M, dtype=jnp.int32), M)
    green = green_values(freq[:, None, None], freq[None, :, None], freq[None, None, :], M)
    return jnp.real(jnp.fft.ifftn(green * jnp.fft.fftn(density))).astype(jnp.float32)


def reference(descriptors, types, offsets, stencil_base, w_first, w_second, w_out, hardness, sr_first, sr_charge, sr_out):
    onehot = (types[None, :] == jnp.arange(ELEMENTS, dtype=jnp.int32)[:, None]).astype(jnp.float32)
    chi = element_net(w_first, w_second, w_out, descriptors, onehot)
    atom_hardness = jnp.sum(onehot * hardness[:, None], axis=0)
    weights, slopes = spline_tables(offsets)
    cells = brick_cells(stencil_base)
    total_atoms = float(ATOMS)

    def operate(values):
        field = poisson(spread(values, cells, weights))
        return atom_hardness * values + sample(field, cells, weights[0], weights[1], weights[2])

    residual = jnp.sum(chi) / total_atoms - chi
    direction = residual
    norm_now = jnp.sum(residual * residual)
    charges = jnp.zeros((ATOMS,), jnp.float32)
    for iteration in range(ITERS):
        image = operate(direction)
        step_size = norm_now / jnp.sum(direction * image)
        charges = charges + step_size * direction
        residual = residual - step_size * (image - jnp.sum(image) / total_atoms)
        if iteration + 1 < ITERS:
            norm_next = jnp.sum(residual * residual)
            direction = residual + (norm_next / norm_now) * direction
            norm_now = norm_next
    potential = poisson(spread(charges, cells, weights))
    forces = -charges[None, :] * jnp.stack([
        sample(potential, cells, slopes[0], weights[1], weights[2]),
        sample(potential, cells, weights[0], slopes[1], weights[2]),
        sample(potential, cells, weights[0], weights[1], slopes[2])])
    hidden = jnp.tanh(jnp.einsum('ehf,fa->eha', sr_first, descriptors, precision=lax.Precision.HIGHEST) + sr_charge[:, :, None] * charges[None, None, :])
    short_energy = jnp.sum(onehot * jnp.einsum('eh,eha->ea', sr_out, hidden, precision=lax.Precision.HIGHEST), axis=0)
    return charges, forces, short_energy
```

```python
import functools
import math

import jax
import jax.numpy as jnp
import numpy as np
from jax import lax
from jax.experimental import pallas as pl
from jax.experimental.pallas import tpu as pltpu
from jax.sharding import PartitionSpec as P

M = 192
SMEAR = 0.75
GX, PAX, QAX = "gx", "gy", "gz"
P_DIM, Q_DIM = 1, 2
AXES = ("gx", "gy", "gz")
ATOMS = 8192
CH = 512
NCH = ATOMS // CH
XR = 56
LN = 256
F32, BF16 = jnp.float32, jnp.bfloat16
MESH = pl.DeviceIdType.MESH


def cas(rows, columns):
    angle = 2.0 * np.pi * ((rows[:, None] * columns[None, :]) % M) / M
    return np.cos(angle) + np.sin(angle)


def halves(array):
    array = np.asarray(array, np.float32)
    high = array.astype(jnp.bfloat16)
    low = (array - high.astype(np.float32)).astype(jnp.bfloat16)
    return np.stack([high, low])


def tables():
    freq = np.arange(M)
    cell_x = (48 * np.arange(4)[:, None] + np.arange(XR)[None, :] - 2).reshape(-1) % M
    real_x = np.tile(np.arange(XR) < 52, 4)
    h_x = cas(freq, cell_x) * real_x[None, :]
    cell_p = (24 * np.arange(8)[:, None] + np.arange(32)[None, :] - 2).reshape(-1) % M
    real_p = np.tile(np.arange(32) < 28, 8)
    row_p = np.arange(M)
    freq_p = (row_p % 32) * 6 + row_p // 32
    h_p = np.zeros((256, 256))
    h_p[:M] = cas(freq_p, cell_p) * real_p[None, :]
    src = np.arange(256) // 8
    part = np.arange(256) % 8
    cell_q = (24 * (src % 8) + 7 * (src // 8) + part - 2) % M
    h_q = cas(freq, cell_q) * (part < 7)[None, :]
    lanes = np.zeros((8, 256), np.float32)
    lanes[0, :144] = np.arange(144) // 24
    lanes[1, :144] = np.arange(144) % 24
    return halves(h_x), halves(h_x.T), halves(h_p), halves(h_q), halves(h_q.T), lanes


def split(value):
    high = value.astype(BF16)
    return high, (value - high.astype(F32)).astype(BF16)


def dot(left, right, dims=((1,), (0,))):
    return lax.dot_general(left, right, (dims, ((), ())), preferred_element_type=F32)


def dot3(table, value, dims=((1,), (0,))):
    high, low = split(value)
    return dot(table[0], high, dims) + (dot(table[0], low, dims) + dot(table[1], high, dims))


def signed(number):
    return jnp.where(2.0 * number >= M, number - M, number)


def peers_x(ix, iq):
    return [(step, {GX: lax.rem(ix + step, 4)}, lax.rem(ix + step, 4)) for step in (2, 1, 3)]


def peers_p(ip):
    return [(step, {PAX: lax.rem(ip + step, 8)}, lax.rem(ip + step, 8)) for step in (4, 3, 5, 2, 6, 1, 7)]


def peers_q(iq):
    return [(step, {QAX: lax.rem(iq + step, 8)}, lax.rem(iq + step, 8)) for step in (4, 3, 5, 2, 6, 1, 7)]


def peers_xq(ix, iq):
    steps = sorted(
        [(a, b) for a in range(4) for b in range(8) if a or b],
        key=lambda t: -(min(t[0], 4 - t[0]) + min(t[1], 8 - t[1])),
    )
    found = []
    for a, b in steps:
        g, h = lax.rem(ix + a, 4), lax.rem(iq + b, 8)
        found.append((a * 8 + b, {GX: g, QAX: h}, g * 8 + h))
    return found


def send_all(peers, src_of, dst, send, recv, base):
    copies = []
    for step, where, number in peers:
        copy = pltpu.make_async_remote_copy(
            src_ref=src_of(number),
            dst_ref=dst,
            send_sem=send.at[base + step],
            recv_sem=recv.at[base + step],
            device_id=where,
            device_id_type=MESH,
        )
        copy.start()
        copies.append(copy)
    return copies


def wait_all(copies):
    for copy in copies:
        copy.wait_recv()
    for copy in copies:
        copy.wait_send()


def rows8(start):
    return pl.ds(pl.multiple_of(start, 8), 8)


def comb_store(ref, row, value):
    for h in range(2):
        ref[h, pl.ds(row, 32, stride=8), :] = value[:, 128 * h : 128 * h + 128]


def lane_pick(pieces, width, length=LN):
    lane = lax.broadcasted_iota(jnp.int32, pieces[0][0].shape, 1)
    result = jnp.zeros(pieces[0][0].shape, F32)
    for number, (array, shift) in enumerate(pieces):
        shift = shift % length
        moved = array if shift == 0 else pltpu.roll(array, shift, 1)
        inside = (lane >= number * width) & (lane < (number + 1) * width)
        result = jnp.where(inside, moved, result)
    return result


def kernel(
    chi_ref, types_ref, offs_ref, base_ref, hard_ref,
    hx_ref, hxt_ref, hp_ref, hq_ref, hqt_ref, lanes_ref,
    charges_ref, forces_ref,
    w_ref, s_ref, mx_ref, mp_ref, mq_ref, a_ref, b_ref, acc_ref,
    ones_ref, sp_ref, sd_ref, r1_ref, k1_ref, r2_ref, x2_ref, m_ref, r3_ref, green_ref,
    z3_ref, r3b_ref, k3b_ref, m2b_ref, r2b_ref, v1_ref, r1b_ref, phi0_ref, phi_ref,
    image_ref, p0_ref, d1_ref, t_ref, arx_ref, arp_ref, arq_ref, ars_ref,
    send, recv,
):
    ix, ip, iq = lax.axis_index(GX), lax.axis_index(PAX), lax.axis_index(QAX)
    mine = ix * 8 + iq
    to_x, to_p, to_q, to_xq = peers_x(ix, iq), peers_p(ip), peers_q(iq), peers_xq(ix, iq)
    barrier = pltpu.get_barrier_semaphore()
    for _, where, _ in to_xq + to_p:
        pl.semaphore_signal(barrier, inc=1, device_id=where, device_id_type=MESH)

    hardness = jnp.where(
        types_ref[...] == 0, hard_ref[0], jnp.where(types_ref[...] == 1, hard_ref[1], hard_ref[2])
    )
    for d in range(3):
        t = offs_ref[d]
        spline = [t, 1.0 - t]
        for order in (3, 4, 5):
            grown = []
            for k in range(order):
                term = None
                if k < order - 1:
                    term = (t + k) * spline[k]
                if k >= 1:
                    other = (order - k - t) * spline[k - 1]
                    term = other if term is None else term + other
                grown.append(term * (1.0 / (order - 1)))
            if order == 5:
                s_ref[d, 0] = -spline[3]
                s_ref[d, 1] = spline[3] - spline[2]
                s_ref[d, 2] = spline[2] - spline[1]
                s_ref[d, 3] = spline[1] - spline[0]
                s_ref[d, 4] = spline[0]
            spline = grown
        for j in range(5):
            w_ref[d, j] = spline[4 - j]

    row = lax.broadcasted_iota(jnp.int32, (M, LN), 0).astype(F32)
    f_q = signed(row)
    f_p = signed(lanes_ref[0:1, :] + (6 * mine).astype(F32))
    f_x = signed(lanes_ref[1:2, :] + (24 * ip).astype(F32))
    factor = 2.0 * math.pi / M
    wave = (factor * factor) * (f_q * f_q + (f_p * f_p + f_x * f_x))
    safe = jnp.where(wave > 0, wave, 1.0)
    green_ref[...] = jnp.where(
        wave > 0, (4.0 * math.pi / (M * M * M)) * jnp.exp((-0.5 * SMEAR * SMEAR) * wave) / safe, 0.0
    )

    zero8 = jnp.zeros((8, LN), F32)
    for g in range(4):
        r1b_ref[g, XR : XR + 8, :] = zero8
        acc_ref[256 * g + 224 : 256 * g + 256, :] = jnp.zeros((32, 256), F32)
    x2_ref[168:256, :] = jnp.zeros((88, LN), F32)
    comb_store(m_ref, 7, jnp.zeros((32, LN), F32))
    k3b_ref[192:256, :] = jnp.zeros((64, LN), F32)

    def mask(table, d, c, count):
        base = base_ref[d, pl.ds(c, 1), :]
        place = lax.broadcasted_iota(jnp.int32, (count, CH), 0) - base
        result = jnp.zeros((count, CH), F32)
        for j in range(5):
            result = jnp.where(place == j, table[d, j, pl.ds(c, 1), :], result)
        return result

    def spread(values_ref, shift, lo, hi, first):
        def step(c, carry):
            if first:
                m_x, m_p, m_q = mask(w_ref, 0, c, 64), mask(w_ref, P_DIM, c, 32), mask(w_ref, Q_DIM, c, 32)
                mx_ref[c], mp_ref[c], mq_ref[c] = m_x, m_p, m_q
                for q in range(28):
                    high, low = split(m_p * m_q[q : q + 1, :])
                    a_ref[c, 32 * q : 32 * q + 32, :] = high
                    a_ref[c, 896 + 32 * q : 896 + 32 * q + 32, :] = low
                b_ref[128:192, :], b_ref[192:256, :] = split(m_x)
            else:
                m_x = mx_ref[c]
            b_ref[0:64, :], b_ref[64:128, :] = split(m_x * (values_ref[pl.ds(c, 1), :] - shift))
            width = 256 if first else 128
            part = dot(a_ref[c], b_ref[0:width, :], ((1,), (1,)))
            for g in range(4):
                acc_ref[256 * g : 256 * g + 224, 0:width] += (
                    part[224 * g : 224 * g + 224] + part[896 + 224 * g : 896 + 224 * g + 224]
                )
            return carry

        lax.fori_loop(lo, hi, step, 0)

    def clear(width):
        for g in range(4):
            acc_ref[256 * g : 256 * g + 224, 0:width] = jnp.zeros((224, width), F32)

    lane = lax.broadcasted_iota(jnp.int32, (8, 128), 1)

    def pack(sums):
        tile = jnp.zeros((8, 128), F32)
        for k, value in enumerate(sums):
            tile = jnp.where(lane == k, value, tile)
        return tile

    def total(array):
        return jnp.sum(jnp.sum(array, axis=0, keepdims=True), axis=1, keepdims=True)

    def ar_start(phase, tile):
        peers, slots, me, base = (
            (to_x, arx_ref, ix, 100), (to_p, arp_ref, ip, 104), (to_q, arq_ref, iq, 112)
        )[phase]
        slots[me] = tile
        ars_ref[phase] = tile
        return send_all(peers, lambda number: ars_ref.at[phase], slots.at[me], send, recv, base)

    def ar_done(phase, copies):
        wait_all(copies)
        return jnp.sum((arx_ref, arp_ref, arq_ref)[phase][...], axis=0)

    def solve():
        r1_ref[ix] = sd_ref[ix, 0:XR, :]
        copies = send_all(to_x, lambda g: sd_ref.at[g, 0:XR], r1_ref.at[ix], send, recv, 0)
        wait_all(copies)
        k1 = dot3(hx_ref, r1_ref[...].reshape(4 * XR, LN))
        k1_ref[...] = k1.reshape(8, 24, LN)
        r2_ref[ip] = k1_ref[ip]
        copies = send_all(to_p, lambda s: k1_ref.at[s], r2_ref.at[ip], send, recv, 4)
        wait_all(copies)
        for y in range(7):
            x2_ref[24 * y : 24 * y + 24, :] = lane_pick(
                [(r2_ref[s], 32 * (s - y)) for s in range(8)], 32
            )
        k2 = dot3((hp_ref[0, 0:M, :], hp_ref[1, 0:M, :]), x2_ref[...], ((1,), (1,)))
        for y in range(7):
            comb_store(
                m_ref,
                y,
                lane_pick([(k2[32 * k : 32 * k + 32, :], 24 * (k - y)) for k in range(6)], 24),
            )
        r3_ref[:, rows8(8 * mine), :] = m_ref[:, rows8(8 * mine), :]
        copies = send_all(
            to_xq, lambda n: m_ref.at[:, rows8(8 * n)], r3_ref.at[:, rows8(8 * mine)], send, recv, 12
        )
        wait_all(copies)
        k3 = dot3(hq_ref, jnp.concatenate([r3_ref[0], r3_ref[1]], axis=1)) * green_ref[...]
        z3 = dot3(hqt_ref, k3)
        z3_ref[0], z3_ref[1] = z3[:, 0:128], z3[:, 128:256]
        r3b_ref[:, rows8(8 * mine), :] = z3_ref[:, rows8(8 * mine), :]
        copies = send_all(
            to_xq, lambda n: z3_ref.at[:, rows8(8 * n)], r3b_ref.at[:, rows8(8 * mine)], send, recv, 44
        )
        wait_all(copies)
        loaded = [
            jnp.concatenate([r3b_ref[h, pl.ds(y, 32, stride=8), :] for h in range(2)], axis=1)
            for y in range(7)
        ]
        for k in range(6):
            k3b_ref[32 * k : 32 * k + 32, :] = lane_pick(
                [(loaded[y], 24 * (y - k)) for y in range(7)], 24
            )
        turned = jnp.transpose(k3b_ref[...])
        high, low = split(turned)
        v2 = dot(high, hp_ref[0]) + (dot(low, hp_ref[0]) + dot(high, hp_ref[1]))
        for s in range(8):
            m2b_ref[s] = lane_pick(
                [(v2[24 * y : 24 * y + 24, :], 32 * (y - s)) for y in range(7)], 32
            )
        r2b_ref[ip] = m2b_ref[ip]
        copies = send_all(to_p, lambda s: m2b_ref.at[s], r2b_ref.at[ip], send, recv, 76)
        wait_all(copies)
        v1_ref[...] = dot3(hxt_ref, r2b_ref[...].reshape(M, LN)).reshape(4, XR, LN)
        r1b_ref[ix, 0:XR, :] = v1_ref[ix]
        copies = send_all(to_x, lambda g: v1_ref.at[g], r1b_ref.at[ix, 0:XR], send, recv, 84)
        wait_all(copies)

    def load_field(get):
        for g in range(4):
            high, low = split(get(g))
            both = jnp.concatenate([high.astype(F32), low.astype(F32)], axis=0)
            turned = jnp.transpose(both)[0:224, :].astype(BF16)
            phi_ref[224 * g : 224 * g + 224, 0:128] = turned
            phi_ref[224 * g : 224 * g + 224, 128:256] = turned

    def x_contract(m_x, slot):
        high, low = split(m_x)
        b_ref[0:64, :], b_ref[64:128, :], b_ref[128:192, :], b_ref[192:256, :] = high, high, low, low
        t_ref[slot] = dot(phi_ref[...], b_ref[...])

    def fold(product):
        return (product[0:8] + product[8:16]) + (product[16:24] + product[24:32])

    def sample_image(values_ref):
        def step(c, carry):
            x_contract(mx_ref[c], 0)
            m_p = mp_ref[c]
            found = jnp.zeros((8, CH), F32)
            for q in range(28):
                found = found + fold(t_ref[0, 32 * q : 32 * q + 32, :] * m_p) * mq_ref[c, q : q + 1, :]
            image_ref[pl.ds(c, 1), :] = jnp.sum(found, axis=0, keepdims=True)
            return carry

        lax.fori_loop(0, NCH, step, 0)
        image_ref[...] = image_ref[...] + hardness * values_ref[...]

    def sample_forces():
        def step(c, carry):
            m_p, s_p = mp_ref[c], mask(s_ref, P_DIM, c, 32)
            b = mask(s_ref, Q_DIM, c, 32)
            x_contract(mx_ref[c], 0)
            x_contract(mask(s_ref, 0, c, 64), 1)
            along_x, along_p, along_q = (jnp.zeros((8, CH), F32) for _ in range(3))
            for q in range(28):
                block = t_ref[0, 32 * q : 32 * q + 32, :]
                m_q = mq_ref[c, q : q + 1, :]
                along_q = along_q + fold(block * m_p) * b[q : q + 1, :]
                along_p = along_p + fold(block * s_p) * m_q
                along_x = along_x + fold(t_ref[1, 32 * q : 32 * q + 32, :] * m_p) * m_q
            minus = -charges_ref[pl.ds(c, 1), :]
            forces_ref[0, pl.ds(c, 1), :] = minus * jnp.sum(along_x, axis=0, keepdims=True)
            forces_ref[P_DIM, pl.ds(c, 1), :] = minus * jnp.sum(along_p, axis=0, keepdims=True)
            forces_ref[Q_DIM, pl.ds(c, 1), :] = minus * jnp.sum(along_q, axis=0, keepdims=True)
            return carry

        lax.fori_loop(0, NCH, step, 0)

    atoms = float(ATOMS * 256)
    clear(256)
    chi = chi_ref[...]
    local_sum = total(chi)
    shift = local_sum * (1.0 / ATOMS)
    pl.semaphore_wait(barrier, len(to_xq) + len(to_p))
    copies = ar_start(0, pack([local_sum]))
    spread(chi_ref, shift, 0, 5, True)
    copies = ar_start(1, ar_done(0, copies))
    spread(chi_ref, shift, 5, 11, True)
    copies = ar_start(2, ar_done(1, copies))
    spread(chi_ref, shift, 11, NCH, True)
    mean = ar_done(2, copies)[0:1, 0:1] * (1.0 / atoms)
    for g in range(4):
        turned = jnp.transpose(acc_ref[256 * g : 256 * g + 256, :])
        ones = turned[128:192] + turned[192:256]
        ones_ref[g] = ones
        field = (mean - shift) * ones - (turned[0:64] + turned[64:128])
        sp_ref[g] = field
        sd_ref[g] = field
    p0 = mean - chi
    p0_ref[...] = p0
    solve()
    for g in range(4):
        phi0_ref[g] = r1b_ref[g]
    load_field(lambda g: r1b_ref[g])
    sample_image(p0_ref)

    image = image_ref[...]
    image_sum = total(image)
    shift2 = image_sum * (1.0 / ATOMS)
    sums = pack([total(p0 * p0), total(p0 * image), image_sum, total(image * image), total(p0)])
    clear(128)
    copies = ar_start(0, sums)
    spread(image_ref, shift2, 0, 5, False)
    copies = ar_start(1, ar_done(0, copies))
    spread(image_ref, shift2, 5, 11, False)
    copies = ar_start(2, ar_done(1, copies))
    spread(image_ref, shift2, 11, NCH, False)
    sums = ar_done(2, copies)
    norm0, curve0, image_total, image_square, p0_total = (sums[0:1, k : k + 1] for k in range(5))
    alpha0 = norm0 / curve0
    image_mean = image_total * (1.0 / atoms)
    norm1 = (
        norm0
        - 2.0 * alpha0 * (curve0 - image_mean * p0_total)
        + alpha0 * alpha0 * (image_square - image_mean * image_total)
    )
    beta = norm1 / norm0
    residual = p0 - alpha0 * (image - image_mean)
    d1_ref[...] = residual + beta * p0
    for g in range(4):
        turned = jnp.transpose(acc_ref[256 * g : 256 * g + 256, 0:128])
        sd_ref[g] = (
            (1.0 + beta) * sp_ref[g]
            + (alpha0 * (image_mean - shift2)) * ones_ref[g]
            - alpha0 * (turned[0:64] + turned[64:128])
        )
    solve()
    load_field(lambda g: r1b_ref[g])
    sample_image(d1_ref)
    d1 = d1_ref[...]
    sums = pack([total(residual * residual), total(d1 * image_ref[...])])
    copies = ar_start(0, sums)
    copies = ar_start(1, ar_done(0, copies))
    copies = ar_start(2, ar_done(1, copies))
    sums = ar_done(2, copies)
    alpha1 = sums[0:1, 0:1] / sums[0:1, 1:2]
    charges_ref[...] = alpha0 * p0_ref[...] + alpha1 * d1
    load_field(lambda g: alpha0 * phi0_ref[g] + alpha1 * r1b_ref[g])
    sample_forces()


def equilibrate(chi, types, offsets, stencil_base, hardness):
    tabs = tables()
    vmem = pl.BlockSpec(memory_space=pltpu.VMEM)
    smem = pl.BlockSpec(memory_space=pltpu.SMEM)

    def held(*shape, dtype=F32):
        return pltpu.VMEM(shape, dtype)

    return pl.pallas_call(
        kernel,
        out_shape=(
            jax.ShapeDtypeStruct((NCH, CH), F32),
            jax.ShapeDtypeStruct((3, NCH, CH), F32),
        ),
        in_specs=[vmem] * 4 + [smem] + [vmem] * 6,
        out_specs=(vmem, vmem),
        scratch_shapes=[
            held(3, 5, NCH, CH), held(3, 5, NCH, CH),
            held(NCH, 64, CH), held(NCH, 32, CH), held(NCH, 32, CH),
            held(NCH, 1792, CH, dtype=BF16), held(256, CH, dtype=BF16),
            held(1024, 256),
            held(4, 64, LN), held(4, 64, LN), held(4, 64, LN),
            held(4, XR, LN), held(8, 24, LN), held(8, 24, LN),
            held(256, LN), held(2, 256, 128), held(2, 256, 128), held(M, LN),
            held(2, 256, 128), held(2, 256, 128), held(256, LN),
            held(8, 24, LN), held(8, 24, LN), held(4, XR, LN),
            held(4, 64, LN), held(4, 64, LN), held(896, 256, dtype=BF16),
            held(NCH, CH), held(NCH, CH), held(NCH, CH),
            held(2, 896, CH),
            held(4, 8, 128), held(8, 8, 128), held(8, 8, 128), held(3, 8, 128),
            pltpu.SemaphoreType.DMA((120,)),
            pltpu.SemaphoreType.DMA((120,)),
        ],
        compiler_params=pltpu.CompilerParams(
            collective_id=0, has_side_effects=True, vmem_limit_bytes=60 * 1024 * 1024
        ),
        name="equilibrate",
    )(
        chi.reshape(NCH, CH), types.reshape(NCH, CH), offsets.reshape(3, NCH, CH),
        stencil_base.reshape(3, NCH, CH), hardness, *[jnp.asarray(t) for t in tabs],
    )


def element_net(first, second, final, descriptors, onehot):
    hidden = jnp.tanh(
        jnp.einsum("ehf,fa->eha", first, descriptors, precision=lax.Precision.HIGHEST)
    )
    hidden = jnp.tanh(jnp.einsum("ehg,ega->eha", second, hidden, precision=lax.Precision.HIGHEST))
    output = jnp.einsum("eh,eha->ea", final, hidden, precision=lax.Precision.HIGHEST)
    return jnp.sum(onehot * output, axis=0)


def per_device(
    descriptors, types, offsets, stencil_base, w_first, w_second, w_out, hardness,
    sr_first, sr_charge, sr_out,
):
    elements = w_first.shape[0]
    onehot = (types[None, :] == jnp.arange(elements, dtype=jnp.int32)[:, None]).astype(F32)
    chi = element_net(w_first, w_second, w_out, descriptors, onehot)
    charges, forces = equilibrate(chi, types, offsets, stencil_base, hardness)
    charges = charges.reshape(ATOMS)
    forces = forces.reshape(3, ATOMS)
    hidden = jnp.tanh(
        jnp.einsum("ehf,fa->eha", sr_first, descriptors, precision=lax.Precision.HIGHEST)
        + sr_charge[:, :, None] * charges[None, None, :]
    )
    short_energy = jnp.sum(
        onehot * jnp.einsum("eh,eha->ea", sr_out, hidden, precision=lax.Precision.HIGHEST), axis=0
    )
    return charges, forces, short_energy


def solution(mesh):
    rows, columns = P(AXES), P(None, AXES)
    return jax.shard_map(
        per_device,
        mesh=mesh,
        in_specs=(columns, rows, columns, columns) + (P(),) * 7,
        out_specs=(rows, columns, rows),
        check_vma=False,
    )
```

```python
import functools
import math

import jax
import jax.numpy as jnp
import numpy as np
from jax import lax
from jax.experimental import pallas as pl
from jax.experimental.pallas import tpu as pltpu
from jax.sharding import PartitionSpec as P

M = 192
SMEAR = 0.75
GX, PAX, QAX = "gx", "gy", "gz"
P_DIM, Q_DIM = 1, 2
AXES = ("gx", "gy", "gz")
ATOMS = 8192
CH = 512
NCH = ATOMS // CH
XR = 56
LN = 256
F32, BF16 = jnp.float32, jnp.bfloat16
MESH = pl.DeviceIdType.MESH


def cas(rows, columns):
    angle = 2.0 * np.pi * ((rows[:, None] * columns[None, :]) % M) / M
    return np.cos(angle) + np.sin(angle)


def halves(array):
    array = np.asarray(array, np.float32)
    high = array.astype(jnp.bfloat16)
    low = (array - high.astype(np.float32)).astype(jnp.bfloat16)
    return np.stack([high, low])


def tables():
    freq = np.arange(M)
    cell_x = (48 * np.arange(4)[:, None] + np.arange(XR)[None, :] - 2).reshape(-1) % M
    real_x = np.tile(np.arange(XR) < 52, 4)
    h_x = cas(freq, cell_x) * real_x[None, :]
    cell_p = (24 * np.arange(8)[:, None] + np.arange(32)[None, :] - 2).reshape(-1) % M
    real_p = np.tile(np.arange(32) < 28, 8)
    row_p = np.arange(M)
    freq_p = (row_p % 32) * 6 + row_p // 32
    h_p = np.zeros((256, 256))
    h_p[:M] = cas(freq_p, cell_p) * real_p[None, :]
    src = np.arange(256) // 8
    part = np.arange(256) % 8
    cell_q = (24 * (src % 8) + 7 * (src // 8) + part - 2) % M
    h_q = cas(freq, cell_q) * (part < 7)[None, :]
    lanes = np.zeros((8, 256), np.float32)
    lanes[0, :144] = np.arange(144) // 24
    lanes[1, :144] = np.arange(144) % 24
    return halves(h_x), halves(h_x.T), halves(h_p), halves(h_q), halves(h_q.T), lanes


def split(value):
    high = value.astype(BF16)
    return high, (value - high.astype(F32)).astype(BF16)


def dot(left, right, dims=((1,), (0,))):
    return lax.dot_general(left, right, (dims, ((), ())), preferred_element_type=F32)


def dot3(table, value, dims=((1,), (0,))):
    high, low = split(value)
    return dot(table[0], high, dims) + (dot(table[0], low, dims) + dot(table[1], high, dims))


def signed(number):
    return jnp.where(2.0 * number >= M, number - M, number)


def peers_x(ix, iq):
    return [(step, {GX: lax.rem(ix + step, 4)}, lax.rem(ix + step, 4)) for step in (2, 1, 3)]


def peers_p(ip):
    return [(step, {PAX: lax.rem(ip + step, 8)}, lax.rem(ip + step, 8)) for step in (4, 3, 5, 2, 6, 1, 7)]


def peers_q(iq):
    return [(step, {QAX: lax.rem(iq + step, 8)}, lax.rem(iq + step, 8)) for step in (4, 3, 5, 2, 6, 1, 7)]


def peers_xq(ix, iq):
    steps = sorted(
        [(a, b) for a in range(4) for b in range(8) if a or b],
        key=lambda t: -(min(t[0], 4 - t[0]) + min(t[1], 8 - t[1])),
    )
    found = []
    for a, b in steps:
        g, h = lax.rem(ix + a, 4), lax.rem(iq + b, 8)
        found.append((a * 8 + b, {GX: g, QAX: h}, g * 8 + h))
    return found


def send_all(peers, src_of, dst, send, recv, base):
    copies = []
    for step, where, number in peers:
        copy = pltpu.make_async_remote_copy(
            src_ref=src_of(number),
            dst_ref=dst,
            send_sem=send.at[base + step],
            recv_sem=recv.at[base + step],
            device_id=where,
            device_id_type=MESH,
        )
        copy.start()
        copies.append(copy)
    return copies


def wait_all(copies):
    for copy in copies:
        copy.wait_recv()
    for copy in copies:
        copy.wait_send()


def rows8(start):
    return pl.ds(pl.multiple_of(start, 8), 8)


def comb_store(ref, row, value):
    for h in range(2):
        ref[h, pl.ds(row, 32, stride=8), :] = value[:, 128 * h : 128 * h + 128]


def lane_pick(pieces, width, length=LN):
    lane = lax.broadcasted_iota(jnp.int32, pieces[0][0].shape, 1)
    result = jnp.zeros(pieces[0][0].shape, F32)
    for number, (array, shift) in enumerate(pieces):
        shift = shift % length
        moved = array if shift == 0 else pltpu.roll(array, shift, 1)
        inside = (lane >= number * width) & (lane < (number + 1) * width)
        result = jnp.where(inside, moved, result)
    return result


def kernel(
    desc_ref, types1_ref, offs1_ref, base1_ref, hard_ref,
    wf_ref, ws_ref, wo_ref, sf_ref, sc_ref, so_ref,
    hx_ref, hxt_ref, hp_ref, hq_ref, hqt_ref, lanes_ref,
    out_charges_ref, out_forces_ref, out_short_ref,
    w_ref, s_ref, mx_ref, mp_ref, mq_ref, a_ref, b_ref, acc_ref,
    ones_ref, sp_ref, sd_ref, r1_ref, k1_ref, r2_ref, x2_ref, m_ref, r3_ref, green_ref,
    z3_ref, r3b_ref, k3b_ref, m2b_ref, r2b_ref, v1_ref, r1b_ref, phi0_ref, phi_ref,
    image_ref, p0_ref, d1_ref, t_ref, arx_ref, arp_ref, arq_ref, ars_ref,
    types_ref, offs_ref, base_ref, chi_ref, charges_ref, pre_ref, n1_ref, n2_ref, n3_ref, tall_ref,
    send, recv,
):
    ix, ip, iq = lax.axis_index(GX), lax.axis_index(PAX), lax.axis_index(QAX)
    mine = ix * 8 + iq
    to_x, to_p, to_q, to_xq = peers_x(ix, iq), peers_p(ip), peers_q(iq), peers_xq(ix, iq)
    barrier = pltpu.get_barrier_semaphore()
    for _, where, _ in to_xq + to_p:
        pl.semaphore_signal(barrier, inc=1, device_id=where, device_id_type=MESH)

    def part(c):
        return pl.ds(c * CH, CH)

    for c in range(NCH):
        types_ref[c : c + 1, :] = types1_ref[:, c * CH : c * CH + CH]
        for d in range(3):
            offs_ref[d, c : c + 1, :] = offs1_ref[d : d + 1, c * CH : c * CH + CH]
            base_ref[d, c : c + 1, :] = base1_ref[d : d + 1, c * CH : c * CH + CH]

    n1_ref[...] = jnp.zeros(n1_ref.shape, F32)
    n2_ref[...] = jnp.zeros(n2_ref.shape, F32)
    n3_ref[...] = jnp.zeros(n3_ref.shape, F32)
    tall_ref[...] = jnp.zeros(tall_ref.shape, F32)
    for e in range(3):
        n1_ref[32 * e : 32 * e + 25, :] = wf_ref[e]
        n1_ref[96 + 32 * e : 96 + 32 * e + 25, :] = sf_ref[e]
        n2_ref[32 * e : 32 * e + 25, 0:25] = ws_ref[e]
    n3_ref[0:3, 0:25] = wo_ref[...]
    n3_ref[8:11, 0:25] = so_ref[...]
    tall_ref[0:3, 0:25] = sc_ref[...]
    tall_ref[...] = jnp.transpose(tall_ref[...])
    first_layer, second_layer = split(n1_ref[...]), split(n2_ref[...])
    last_layer, short_layer = split(n3_ref[0:8, :]), split(n3_ref[8:16, :])

    def by_type(c, first, second, third):
        kind = types_ref[pl.ds(c, 1), :]
        return jnp.where(kind == 0, first, jnp.where(kind == 1, second, third))

    def net_start(c, carry):
        pre = dot3(first_layer, desc_ref[:, part(c)])
        pre_ref[c] = by_type(c, pre[96:128], pre[128:160], pre[160:192])
        hidden = jnp.tanh(by_type(c, pre[0:32], pre[32:64], pre[64:96]))
        pre = dot3(second_layer, hidden)
        hidden = jnp.tanh(by_type(c, pre[0:32], pre[32:64], pre[64:96]))
        value = dot3(last_layer, hidden)
        chi_ref[pl.ds(c, 1), :] = by_type(c, value[0:1], value[1:2], value[2:3])
        return carry

    def net_end(c, carry):
        charge = charges_ref[pl.ds(c, 1), :]
        weight = by_type(c, tall_ref[0:32, 0:1], tall_ref[0:32, 1:2], tall_ref[0:32, 2:3])
        hidden = jnp.tanh(pre_ref[c] + weight * charge)
        value = dot3(short_layer, hidden)
        out_short_ref[:, part(c)] = by_type(c, value[0:1], value[1:2], value[2:3])
        out_charges_ref[:, part(c)] = charge
        return carry

    hardness = jnp.where(
        types_ref[...] == 0, hard_ref[0], jnp.where(types_ref[...] == 1, hard_ref[1], hard_ref[2])
    )
    for d in range(3):
        t = offs_ref[d]
        spline = [t, 1.0 - t]
        for order in (3, 4, 5):
            grown = []
            for k in range(order):
                term = None
                if k < order - 1:
                    term = (t + k) * spline[k]
                if k >= 1:
                    other = (order - k - t) * spline[k - 1]
                    term = other if term is None else term + other
                grown.append(term * (1.0 / (order - 1)))
            if order == 5:
                s_ref[d, 0] = -spline[3]
                s_ref[d, 1] = spline[3] - spline[2]
                s_ref[d, 2] = spline[2] - spline[1]
                s_ref[d, 3] = spline[1] - spline[0]
                s_ref[d, 4] = spline[0]
            spline = grown
        for j in range(5):
            w_ref[d, j] = spline[4 - j]

    row = lax.broadcasted_iota(jnp.int32, (M, LN), 0).astype(F32)
    f_q = signed(row)
    f_p = signed(lanes_ref[0:1, :] + (6 * mine).astype(F32))
    f_x = signed(lanes_ref[1:2, :] + (24 * ip).astype(F32))
    factor = 2.0 * math.pi / M
    wave = (factor * factor) * (f_q * f_q + (f_p * f_p + f_x * f_x))
    safe = jnp.where(wave > 0, wave, 1.0)
    green_ref[...] = jnp.where(
        wave > 0, (4.0 * math.pi / (M * M * M)) * jnp.exp((-0.5 * SMEAR * SMEAR) * wave) / safe, 0.0
    )

    zero8 = jnp.zeros((8, LN), F32)
    for g in range(4):
        r1b_ref[g, XR : XR + 8, :] = zero8
        acc_ref[256 * g + 224 : 256 * g + 256, :] = jnp.zeros((32, 256), F32)
    x2_ref[168:256, :] = jnp.zeros((88, LN), F32)
    comb_store(m_ref, 7, jnp.zeros((32, LN), F32))
    k3b_ref[192:256, :] = jnp.zeros((64, LN), F32)

    def mask(table, d, c, count):
        base = base_ref[d, pl.ds(c, 1), :]
        place = lax.broadcasted_iota(jnp.int32, (count, CH), 0) - base
        result = jnp.zeros((count, CH), F32)
        for j in range(5):
            result = jnp.where(place == j, table[d, j, pl.ds(c, 1), :], result)
        return result

    def spread(values_ref, shift, lo, hi, first):
        def step(c, carry):
            if first:
                m_x, m_p, m_q = mask(w_ref, 0, c, 64), mask(w_ref, P_DIM, c, 32), mask(w_ref, Q_DIM, c, 32)
                mx_ref[c], mp_ref[c], mq_ref[c] = m_x, m_p, m_q
                for q in range(28):
                    high, low = split(m_p * m_q[q : q + 1, :])
                    a_ref[c, 32 * q : 32 * q + 32, :] = high
                    a_ref[c, 896 + 32 * q : 896 + 32 * q + 32, :] = low
                b_ref[128:192, :], b_ref[192:256, :] = split(m_x)
            else:
                m_x = mx_ref[c]
            b_ref[0:64, :], b_ref[64:128, :] = split(m_x * (values_ref[pl.ds(c, 1), :] - shift))
            width = 256 if first else 128
            part = dot(a_ref[c], b_ref[0:width, :], ((1,), (1,)))
            for g in range(4):
                acc_ref[256 * g : 256 * g + 224, 0:width] += (
                    part[224 * g : 224 * g + 224] + part[896 + 224 * g : 896 + 224 * g + 224]
                )
            return carry

        lax.fori_loop(lo, hi, step, 0)

    def clear(width):
        for g in range(4):
            acc_ref[256 * g : 256 * g + 224, 0:width] = jnp.zeros((224, width), F32)

    lane = lax.broadcasted_iota(jnp.int32, (8, 128), 1)

    def pack(sums):
        tile = jnp.zeros((8, 128), F32)
        for k, value in enumerate(sums):
            tile = jnp.where(lane == k, value, tile)
        return tile

    def total(array):
        return jnp.sum(jnp.sum(array, axis=0, keepdims=True), axis=1, keepdims=True)

    def ar_start(phase, tile):
        peers, slots, me, base = (
            (to_x, arx_ref, ix, 100), (to_p, arp_ref, ip, 104), (to_q, arq_ref, iq, 112)
        )[phase]
        slots[me] = tile
        ars_ref[phase] = tile
        return send_all(peers, lambda number: ars_ref.at[phase], slots.at[me], send, recv, base)

    def ar_done(phase, copies):
        wait_all(copies)
        return jnp.sum((arx_ref, arp_ref, arq_ref)[phase][...], axis=0)

    def solve(local_sums=None):
        r1_ref[ix] = sd_ref[ix, 0:XR, :]
        copies = send_all(to_x, lambda g: sd_ref.at[g, 0:XR], r1_ref.at[ix], send, recv, 0)
        wait_all(copies)
        k1 = dot3(hx_ref, r1_ref[...].reshape(4 * XR, LN))
        k1_ref[...] = k1.reshape(8, 24, LN)
        r2_ref[ip] = k1_ref[ip]
        copies = send_all(to_p, lambda s: k1_ref.at[s], r2_ref.at[ip], send, recv, 4)
        wait_all(copies)
        for y in range(7):
            x2_ref[24 * y : 24 * y + 24, :] = lane_pick(
                [(r2_ref[s], 32 * (s - y)) for s in range(8)], 32
            )
        k2 = dot3((hp_ref[0, 0:M, :], hp_ref[1, 0:M, :]), x2_ref[...], ((1,), (1,)))
        for y in range(7):
            comb_store(
                m_ref,
                y,
                lane_pick([(k2[32 * k : 32 * k + 32, :], 24 * (k - y)) for k in range(6)], 24),
            )
        r3_ref[:, rows8(8 * mine), :] = m_ref[:, rows8(8 * mine), :]
        copies = send_all(
            to_xq, lambda n: m_ref.at[:, rows8(8 * n)], r3_ref.at[:, rows8(8 * mine)], send, recv, 12
        )
        wait_all(copies)
        k3 = dot3(hq_ref, jnp.concatenate([r3_ref[0], r3_ref[1]], axis=1))
        energy_density = k3 * k3 * green_ref[...]
        k3 = k3 * green_ref[...]
        z3 = dot3(hqt_ref, k3)
        z3_ref[0], z3_ref[1] = z3[:, 0:128], z3[:, 128:256]
        r3b_ref[:, rows8(8 * mine), :] = z3_ref[:, rows8(8 * mine), :]
        copies = send_all(
            to_xq, lambda n: z3_ref.at[:, rows8(8 * n)], r3b_ref.at[:, rows8(8 * mine)], send, recv, 44
        )
        if local_sums is not None:
            sums = ar_start(0, pack(local_sums(total(energy_density))))
        wait_all(copies)
        loaded = [
            jnp.concatenate([r3b_ref[h, pl.ds(y, 32, stride=8), :] for h in range(2)], axis=1)
            for y in range(7)
        ]
        for k in range(6):
            k3b_ref[32 * k : 32 * k + 32, :] = lane_pick(
                [(loaded[y], 24 * (y - k)) for y in range(7)], 24
            )
        turned = jnp.transpose(k3b_ref[...])
        high, low = split(turned)
        v2 = dot(high, hp_ref[0]) + (dot(low, hp_ref[0]) + dot(high, hp_ref[1]))
        for s in range(8):
            m2b_ref[s] = lane_pick(
                [(v2[24 * y : 24 * y + 24, :], 32 * (y - s)) for y in range(7)], 32
            )
        r2b_ref[ip] = m2b_ref[ip]
        copies = send_all(to_p, lambda s: m2b_ref.at[s], r2b_ref.at[ip], send, recv, 76)
        if local_sums is not None:
            sums = ar_start(1, ar_done(0, sums))
        wait_all(copies)
        v1_ref[...] = dot3(hxt_ref, r2b_ref[...].reshape(M, LN)).reshape(4, XR, LN)
        r1b_ref[ix, 0:XR, :] = v1_ref[ix]
        copies = send_all(to_x, lambda g: v1_ref.at[g], r1b_ref.at[ix, 0:XR], send, recv, 84)
        if local_sums is not None:
            sums = ar_start(2, ar_done(1, sums))
        wait_all(copies)
        return None if local_sums is None else ar_done(2, sums)

    def load_field(get):
        for g in range(4):
            high, low = split(get(g))
            both = jnp.concatenate([high.astype(F32), low.astype(F32)], axis=0)
            turned = jnp.transpose(both)[0:224, :].astype(BF16)
            phi_ref[224 * g : 224 * g + 224, 0:128] = turned
            phi_ref[224 * g : 224 * g + 224, 128:256] = turned

    def x_contract(m_x, slot):
        high, low = split(m_x)
        b_ref[0:64, :], b_ref[64:128, :], b_ref[128:192, :], b_ref[192:256, :] = high, high, low, low
        t_ref[slot] = dot(phi_ref[...], b_ref[...])

    def fold(product):
        return (product[0:8] + product[8:16]) + (product[16:24] + product[24:32])

    def sample_image(values_ref):
        def step(c, carry):
            x_contract(mx_ref[c], 0)
            m_p = mp_ref[c]
            found = jnp.zeros((8, CH), F32)
            for q in range(28):
                found = found + fold(t_ref[0, 32 * q : 32 * q + 32, :] * m_p) * mq_ref[c, q : q + 1, :]
            image_ref[pl.ds(c, 1), :] = jnp.sum(found, axis=0, keepdims=True)
            return carry

        lax.fori_loop(0, NCH, step, 0)
        image_ref[...] = image_ref[...] + hardness * values_ref[...]

    def sample_forces():
        def step(c, carry):
            m_p, s_p = mp_ref[c], mask(s_ref, P_DIM, c, 32)
            b = mask(s_ref, Q_DIM, c, 32)
            x_contract(mx_ref[c], 0)
            x_contract(mask(s_ref, 0, c, 64), 1)
            along_x, along_p, along_q = (jnp.zeros((8, CH), F32) for _ in range(3))
            for q in range(28):
                block = t_ref[0, 32 * q : 32 * q + 32, :]
                m_q = mq_ref[c, q : q + 1, :]
                along_q = along_q + fold(block * m_p) * b[q : q + 1, :]
                along_p = along_p + fold(block * s_p) * m_q
                along_x = along_x + fold(t_ref[1, 32 * q : 32 * q + 32, :] * m_p) * m_q
            minus = -charges_ref[pl.ds(c, 1), :]
            for d, along in ((0, along_x), (P_DIM, along_p), (Q_DIM, along_q)):
                out_forces_ref[d : d + 1, part(c)] = minus * jnp.sum(along, axis=0, keepdims=True)
            return carry

        lax.fori_loop(0, NCH, step, 0)

    atoms = float(ATOMS * 256)
    clear(256)
    lax.fori_loop(0, NCH, net_start, 0)
    chi = chi_ref[...]
    local_sum = total(chi)
    shift = local_sum * (1.0 / ATOMS)
    pl.semaphore_wait(barrier, len(to_xq) + len(to_p))
    copies = ar_start(0, pack([local_sum]))
    spread(chi_ref, shift, 0, 5, True)
    copies = ar_start(1, ar_done(0, copies))
    spread(chi_ref, shift, 5, 11, True)
    copies = ar_start(2, ar_done(1, copies))
    spread(chi_ref, shift, 11, NCH, True)
    mean = ar_done(2, copies)[0:1, 0:1] * (1.0 / atoms)
    for g in range(4):
        turned = jnp.transpose(acc_ref[256 * g : 256 * g + 256, :])
        ones = turned[128:192] + turned[192:256]
        ones_ref[g] = ones
        field = (mean - shift) * ones - (turned[0:64] + turned[64:128])
        sp_ref[g] = field
        sd_ref[g] = field
    p0 = mean - chi
    p0_ref[...] = p0
    solve()
    for g in range(4):
        phi0_ref[g] = r1b_ref[g]
    load_field(lambda g: r1b_ref[g])
    sample_image(p0_ref)

    image = image_ref[...]
    image_sum = total(image)
    shift2 = image_sum * (1.0 / ATOMS)
    sums = pack([total(p0 * p0), total(p0 * image), image_sum, total(image * image), total(p0)])
    clear(128)
    copies = ar_start(0, sums)
    spread(image_ref, shift2, 0, 5, False)
    copies = ar_start(1, ar_done(0, copies))
    spread(image_ref, shift2, 5, 11, False)
    copies = ar_start(2, ar_done(1, copies))
    spread(image_ref, shift2, 11, NCH, False)
    sums = ar_done(2, copies)
    norm0, curve0, image_total, image_square, p0_total = (sums[0:1, k : k + 1] for k in range(5))
    alpha0 = norm0 / curve0
    image_mean = image_total * (1.0 / atoms)
    norm1 = (
        norm0
        - 2.0 * alpha0 * (curve0 - image_mean * p0_total)
        + alpha0 * alpha0 * (image_square - image_mean * image_total)
    )
    beta = norm1 / norm0
    residual = p0 - alpha0 * (image - image_mean)
    d1_ref[...] = residual + beta * p0
    for g in range(4):
        turned = jnp.transpose(acc_ref[256 * g : 256 * g + 256, 0:128])
        sd_ref[g] = (
            (1.0 + beta) * sp_ref[g]
            + (alpha0 * (image_mean - shift2)) * ones_ref[g]
            - alpha0 * (turned[0:64] + turned[64:128])
        )
    d1 = d1_ref[...]
    sums = solve(lambda energy: [total(residual * residual), total(hardness * d1 * d1) + energy])
    d1 = d1_ref[...]
    alpha1 = sums[0:1, 0:1] / sums[0:1, 1:2]
    charges_ref[...] = alpha0 * p0_ref[...] + alpha1 * d1
    lax.fori_loop(0, NCH, net_end, 0)
    load_field(lambda g: alpha0 * phi0_ref[g] + alpha1 * r1b_ref[g])
    sample_forces()


def per_device(
    descriptors, types, offsets, stencil_base, w_first, w_second, w_out, hardness,
    sr_first, sr_charge, sr_out,
):
    tabs = tables()
    vmem = pl.BlockSpec(memory_space=pltpu.VMEM)
    smem = pl.BlockSpec(memory_space=pltpu.SMEM)

    def held(*shape, dtype=F32):
        return pltpu.VMEM(shape, dtype)

    charges, forces, short_energy = pl.pallas_call(
        kernel,
        out_shape=(
            jax.ShapeDtypeStruct((1, ATOMS), F32),
            jax.ShapeDtypeStruct((3, ATOMS), F32),
            jax.ShapeDtypeStruct((1, ATOMS), F32),
        ),
        in_specs=[vmem] * 4 + [smem] + [vmem] * 12,
        out_specs=(vmem, vmem, vmem),
        scratch_shapes=[
            held(3, 5, NCH, CH), held(3, 5, NCH, CH),
            held(NCH, 64, CH), held(NCH, 32, CH), held(NCH, 32, CH),
            held(NCH, 1792, CH, dtype=BF16), held(256, CH, dtype=BF16),
            held(1024, 256),
            held(4, 64, LN), held(4, 64, LN), held(4, 64, LN),
            held(4, XR, LN), held(8, 24, LN), held(8, 24, LN),
            held(256, LN), held(2, 256, 128), held(2, 256, 128), held(M, LN),
            held(2, 256, 128), held(2, 256, 128), held(256, LN),
            held(8, 24, LN), held(8, 24, LN), held(4, XR, LN),
            held(4, 64, LN), held(4, 64, LN), held(896, 256, dtype=BF16),
            held(NCH, CH), held(NCH, CH), held(NCH, CH),
            held(2, 896, CH),
            held(4, 8, 128), held(8, 8, 128), held(8, 8, 128), held(3, 8, 128),
            held(NCH, CH, dtype=jnp.int32), held(3, NCH, CH), held(3, NCH, CH, dtype=jnp.int32),
            held(NCH, CH), held(NCH, CH), held(NCH, 32, CH),
            held(192, 64), held(96, 32), held(16, 32), held(128, 128),
            pltpu.SemaphoreType.DMA((120,)),
            pltpu.SemaphoreType.DMA((120,)),
        ],
        compiler_params=pltpu.CompilerParams(
            collective_id=0, has_side_effects=True, vmem_limit_bytes=60 * 1024 * 1024
        ),
        name="equilibrate",
    )(
        descriptors, types.reshape(1, ATOMS), offsets, stencil_base, hardness,
        w_first, w_second, w_out, sr_first, sr_charge, sr_out,
        *[jnp.asarray(t) for t in tabs],
    )
    return charges.reshape(ATOMS), forces, short_energy.reshape(ATOMS)


def solution(mesh):
    rows, columns = P(AXES), P(None, AXES)
    return jax.shard_map(
        per_device,
        mesh=mesh,
        in_specs=(columns, rows, columns, columns) + (P(),) * 7,
        out_specs=(rows, columns, rows),
        check_vma=False,
    )
```

```python
import functools
import math

import jax
import jax.numpy as jnp
import numpy as np
from jax import lax
from jax.experimental import pallas as pl
from jax.experimental.pallas import tpu as pltpu
from jax.sharding import PartitionSpec as P

M = 192
SMEAR = 0.75
GX, PAX, QAX = "gx", "gz", "gy"
P_DIM, Q_DIM = 2, 1
AXES = ("gx", "gy", "gz")
ATOMS = 8192
CH = 512
NCH = ATOMS // CH
PAIRS = NCH // 2
WIDE = 2048
XR = 56
LN = 256
F32, BF16 = jnp.float32, jnp.bfloat16
MESH = pl.DeviceIdType.MESH


def cas(rows, columns):
    angle = 2.0 * np.pi * ((rows[:, None] * columns[None, :]) % M) / M
    return np.cos(angle) + np.sin(angle)


def halves(array):
    array = np.asarray(array, np.float32)
    high = array.astype(jnp.bfloat16)
    low = (array - high.astype(np.float32)).astype(jnp.bfloat16)
    return np.stack([high, low])


def tables():
    freq = np.arange(M)
    cell_x = (48 * np.arange(4)[:, None] + np.arange(XR)[None, :] - 2).reshape(-1) % M
    real_x = np.tile(np.arange(XR) < 52, 4)
    h_x = cas(freq, cell_x) * real_x[None, :]
    cell_p = (24 * np.arange(8)[:, None] + np.arange(32)[None, :] - 2).reshape(-1) % M
    real_p = np.tile(np.arange(32) < 28, 8)
    row_p = np.arange(M)
    freq_p = (row_p % 32) * 6 + row_p // 32
    h_p = np.zeros((256, 256))
    h_p[:M] = cas(freq_p, cell_p) * real_p[None, :]
    src = np.arange(256) // 8
    part = np.arange(256) % 8
    cell_q = (24 * (src % 8) + 7 * (src // 8) + part - 2) % M
    h_q = cas(freq, cell_q) * (part < 7)[None, :]
    lanes = np.zeros((8, 256), np.float32)
    lanes[0, :144] = np.arange(144) // 24
    lanes[1, :144] = np.arange(144) % 24
    return halves(h_x), halves(h_x.T), halves(h_p), halves(h_q), halves(h_q.T), lanes


def split(value):
    high = value.astype(BF16)
    return high, (value - high.astype(F32)).astype(BF16)


def dot(left, right, dims=((1,), (0,))):
    return lax.dot_general(left, right, (dims, ((), ())), preferred_element_type=F32)


def dot3(table, value, dims=((1,), (0,))):
    high, low = split(value)
    return dot(table[0], high, dims) + (dot(table[0], low, dims) + dot(table[1], high, dims))


def signed(number):
    return jnp.where(2.0 * number >= M, number - M, number)


def peers_x(ix, iq):
    return [(step, {GX: lax.rem(ix + step, 4)}, lax.rem(ix + step, 4)) for step in (2, 1, 3)]


def peers_p(ip):
    return [(step, {PAX: lax.rem(ip + step, 8)}, lax.rem(ip + step, 8)) for step in (4, 3, 5, 2, 6, 1, 7)]


def peers_q(iq):
    return [(step, {QAX: lax.rem(iq + step, 8)}, lax.rem(iq + step, 8)) for step in (4, 3, 5, 2, 6, 1, 7)]


def peers_xq(ix, iq):
    steps = sorted(
        [(a, b) for a in range(4) for b in range(8) if a or b],
        key=lambda t: -(min(t[0], 4 - t[0]) + min(t[1], 8 - t[1])),
    )
    found = []
    for a, b in steps:
        g, h = lax.rem(ix + a, 4), lax.rem(iq + b, 8)
        found.append((a * 8 + b, {GX: g, QAX: h}, g * 8 + h))
    return found


def send_all(peers, src_of, dst, send, recv, base):
    copies = []
    for step, where, number in peers:
        copy = pltpu.make_async_remote_copy(
            src_ref=src_of(number),
            dst_ref=dst,
            send_sem=send.at[base + step],
            recv_sem=recv.at[base + step],
            device_id=where,
            device_id_type=MESH,
        )
        copy.start()
        copies.append(copy)
    return copies


def wait_all(copies):
    for copy in copies:
        copy.wait_recv()
    for copy in copies:
        copy.wait_send()


def rows8(start):
    return pl.ds(pl.multiple_of(start, 8), 8)


def comb(row):
    return pl.ds(row, 32, stride=8)


def turn(value, shift):
    shift = shift % value.shape[1]
    return value if shift == 0 else pltpu.roll(value, shift, 1)


def waits(copies):
    for copy in copies:
        copy.wait_recv()


def lane_pick(pieces, width):
    lane = lax.broadcasted_iota(jnp.int32, pieces[0][0].shape, 1)
    result = jnp.zeros(pieces[0][0].shape, F32)
    for number, (array, shift) in enumerate(pieces):
        inside = (lane >= number * width) & (lane < (number + 1) * width)
        result = jnp.where(inside, turn(array, shift), result)
    return result


def kernel(
    desc_ref, types1_ref, offs1_ref, base1_ref, hard_ref,
    wf_ref, ws_ref, wo_ref, sf_ref, sc_ref, so_ref,
    hx_ref, hxt_ref, hp_ref, hq_ref, hqt_ref, lanes_ref,
    out_charges_ref, out_forces_ref, out_short_ref,
    w_ref, s_ref, mx_ref, mp_ref, mq_ref, bx_ref, sx_ref, sp_mask_ref, sq_mask_ref,
    a0_ref, a1_ref, b0_ref, b1_ref, acc_ref,
    ones_ref, sp_ref, sd_ref, r1_ref, k1_ref, r2_ref, x2_ref, m_ref, r3_ref, r3x_ref, green_ref,
    z3_ref, z3x_ref, r3b_ref, k3b_ref, m2b_ref, r2b_ref, v1_ref, r1b_ref, phi0_ref, phi_ref,
    image_ref, p0_ref, d1_ref, t_ref, arx_ref, arp_ref, arq_ref, ars_ref,
    types_ref, offs_ref, base_ref, chi_ref, charges_ref, pre_ref, n1_ref, n2_ref, n3_ref, tall_ref,
    send, recv,
):
    ix, ip, iq = lax.axis_index(GX), lax.axis_index(PAX), lax.axis_index(QAX)
    mine = ix * 8 + iq
    to_x, to_p, to_q, to_xq = peers_x(ix, iq), peers_p(ip), peers_q(iq), peers_xq(ix, iq)
    barrier = pltpu.get_barrier_semaphore()
    for _, where, _ in to_xq + to_p:
        pl.semaphore_signal(barrier, inc=1, device_id=where, device_id_type=MESH)

    def part(c):
        return pl.ds(c * CH, CH)

    for c in range(NCH):
        types_ref[c : c + 1, :] = types1_ref[:, c * CH : c * CH + CH]
        for d in range(3):
            offs_ref[d, c : c + 1, :] = offs1_ref[d : d + 1, c * CH : c * CH + CH]
            base_ref[d, c : c + 1, :] = base1_ref[d : d + 1, c * CH : c * CH + CH]

    n1_ref[...] = jnp.zeros(n1_ref.shape, F32)
    n2_ref[...] = jnp.zeros(n2_ref.shape, F32)
    n3_ref[...] = jnp.zeros(n3_ref.shape, F32)
    tall_ref[...] = jnp.zeros(tall_ref.shape, F32)
    for e in range(3):
        n1_ref[32 * e : 32 * e + 25, :] = wf_ref[e]
        n1_ref[96 + 32 * e : 96 + 32 * e + 25, :] = sf_ref[e]
        n2_ref[32 * e : 32 * e + 25, 0:25] = ws_ref[e]
    n3_ref[0:3, 0:25] = wo_ref[...]
    n3_ref[8:11, 0:25] = so_ref[...]
    tall_ref[0:3, 0:25] = sc_ref[...]
    tall_ref[...] = jnp.transpose(tall_ref[...])
    first_layer, second_layer = split(n1_ref[...]), split(n2_ref[...])
    last_layer, short_layer = split(n3_ref[0:8, :]), split(n3_ref[8:16, :])

    def wide(i):
        return pl.ds(i * WIDE, WIDE)

    def by_type(i, first, second, third):
        kind = types1_ref[:, wide(i)]
        return jnp.where(kind == 0, first, jnp.where(kind == 1, second, third))

    def net_chi(i, carry):
        pre = dot3([half[0:96] for half in first_layer], desc_ref[:, wide(i)])
        hidden = jnp.tanh(by_type(i, pre[0:32], pre[32:64], pre[64:96]))
        pre = dot3(second_layer, hidden)
        hidden = jnp.tanh(by_type(i, pre[0:32], pre[32:64], pre[64:96]))
        value = dot3(last_layer, hidden)
        value = by_type(i, value[0:1], value[1:2], value[2:3])
        for k in range(WIDE // CH):
            chi_ref[pl.ds(WIDE // CH * i + k, 1), :] = value[:, CH * k : CH * k + CH]
        return carry

    def net_short(i, carry):
        pre = dot3([half[96:192] for half in first_layer], desc_ref[:, wide(i)])
        pre_ref[:, wide(i)] = by_type(i, pre[0:32], pre[32:64], pre[64:96])
        return carry

    def net_end(i, carry):
        rows = [charges_ref[pl.ds(WIDE // CH * i + k, 1), :] for k in range(WIDE // CH)]
        charge = jnp.concatenate(rows, axis=1)
        weight = by_type(i, tall_ref[0:32, 0:1], tall_ref[0:32, 1:2], tall_ref[0:32, 2:3])
        hidden = jnp.tanh(pre_ref[:, wide(i)] + weight * charge)
        value = dot3(short_layer, hidden)
        value = by_type(i, value[0:1], value[1:2], value[2:3])
        for k in range(WIDE // 128):
            row = pl.ds(WIDE // 128 * i + k, 1)
            out_short_ref[row, :] = value[:, 128 * k : 128 * k + 128]
            out_charges_ref[row, :] = charge[:, 128 * k : 128 * k + 128]
        return carry

    hardness = jnp.where(
        types_ref[...] == 0, hard_ref[0], jnp.where(types_ref[...] == 1, hard_ref[1], hard_ref[2])
    )
    for d in range(3):
        t = offs_ref[d]
        spline = [t, 1.0 - t]
        for order in (3, 4, 5):
            grown = []
            for k in range(order):
                term = None
                if k < order - 1:
                    term = (t + k) * spline[k]
                if k >= 1:
                    other = (order - k - t) * spline[k - 1]
                    term = other if term is None else term + other
                grown.append(term * (1.0 / (order - 1)))
            if order == 5:
                s_ref[d, 0] = -spline[3]
                s_ref[d, 1] = spline[3] - spline[2]
                s_ref[d, 2] = spline[2] - spline[1]
                s_ref[d, 3] = spline[1] - spline[0]
                s_ref[d, 4] = spline[0]
            spline = grown
        for j in range(5):
            w_ref[d, j] = spline[4 - j]

    row = lax.broadcasted_iota(jnp.int32, (M, LN), 0).astype(F32)
    f_q = signed(row)
    f_p = signed(lanes_ref[0:1, :] + (6 * mine).astype(F32))
    f_x = signed(lanes_ref[1:2, :] + (24 * ip).astype(F32))
    factor = 2.0 * math.pi / M
    wave = (factor * factor) * (f_q * f_q + (f_p * f_p + f_x * f_x))
    safe = jnp.where(wave > 0, wave, 1.0)
    green_ref[...] = jnp.where(
        wave > 0, (4.0 * math.pi / (M * M * M)) * jnp.exp((-0.5 * SMEAR * SMEAR) * wave) / safe, 0.0
    )

    for g in range(4):
        for h in range(2):
            r1b_ref[h, g, XR : XR + 8, :] = jnp.zeros((8, 128), F32)
        acc_ref[256 * g + 224 : 256 * g + 256, :] = jnp.zeros((32, 256), F32)
    x2_ref[168:256, :] = jnp.zeros((88, LN), F32)
    r3x_ref[comb(7), :] = jnp.zeros((32, 128), F32)
    k3b_ref[192:256, :] = jnp.zeros((64, LN), F32)

    def mask(table, d, c, count):
        base = base_ref[d, pl.ds(c, 1), :]
        place = lax.broadcasted_iota(jnp.int32, (count, CH), 0) - base
        result = jnp.zeros((count, CH), F32)
        for j in range(5):
            result = jnp.where(place == j, table[d, j, pl.ds(c, 1), :], result)
        return result

    def slope_masks(c, carry):
        high, low = split(mask(s_ref, 0, c, 64))
        sx_ref[c, 0:64, :], sx_ref[c, 64:128, :] = high, low
        sp_mask_ref[c], sq_mask_ref[c] = mask(s_ref, P_DIM, c, 32), mask(s_ref, Q_DIM, c, 32)
        return carry

    def build(c, a_ref, i, b_ref, values_ref, shift):
        m_x, m_p, m_q = mask(w_ref, 0, c, 64), mask(w_ref, P_DIM, c, 32), mask(w_ref, Q_DIM, c, 32)
        mx_ref[c], mp_ref[c], mq_ref[c] = m_x, m_p, m_q
        for q in range(28):
            high, low = split(m_p * m_q[q : q + 1, :])
            a_ref[i, 32 * q : 32 * q + 32, :] = high
            a_ref[i, 896 + 32 * q : 896 + 32 * q + 32, :] = low
        high, low = split(m_x)
        b_ref[128:192, :], b_ref[192:256, :] = high, low
        bx_ref[c, 0:64, :], bx_ref[c, 64:128, :] = high, low
        b_ref[0:64, :], b_ref[64:128, :] = split(m_x * (values_ref[pl.ds(c, 1), :] - shift))

    def gather_part(part, width):
        for g in range(4):
            acc_ref[256 * g : 256 * g + 224, 0:width] += (
                part[224 * g : 224 * g + 224] + part[896 + 224 * g : 896 + 224 * g + 224]
            )

    def spread_first(lo, hi):
        def step(i, carry):
            part = dot(a0_ref[i], b0_ref[...], ((1,), (1,)))
            build(2 * i + 1, a1_ref, i, b1_ref, chi_ref, shift)
            gather_part(part, 256)
            part = dot(a1_ref[i], b1_ref[...], ((1,), (1,)))
            after = lax.rem(i + 1, PAIRS)
            build(2 * after, a0_ref, after, b0_ref, chi_ref, shift)
            gather_part(part, 256)
            return carry

        lax.fori_loop(lo, hi, step, 0)

    def spread_image(lo, hi):
        def step(i, carry):
            for c, b_ref in ((2 * i, b0_ref), (2 * i + 1, b1_ref)):
                value = image_ref[pl.ds(c, 1), :] - shift2
                b_ref[0:64, :], b_ref[64:128, :] = split(mx_ref[c] * value)
            part = dot(a0_ref[i], b0_ref[0:128, :], ((1,), (1,)))
            other = dot(a1_ref[i], b1_ref[0:128, :], ((1,), (1,)))
            gather_part(part, 128)
            gather_part(other, 128)
            return carry

        lax.fori_loop(lo, hi, step, 0)

    def clear(width):
        for g in range(4):
            acc_ref[256 * g : 256 * g + 224, 0:width] = jnp.zeros((224, width), F32)

    lane = lax.broadcasted_iota(jnp.int32, (8, 128), 1)

    def pack(sums):
        tile = jnp.zeros((8, 128), F32)
        for k, value in enumerate(sums):
            tile = jnp.where(lane == k, value, tile)
        return tile

    def total(array):
        return jnp.sum(jnp.sum(array, axis=0, keepdims=True), axis=1, keepdims=True)

    def ar_start(phase, tile):
        peers, slots, me, base = (
            (to_x, arx_ref, ix, 112), (to_p, arp_ref, ip, 116), (to_q, arq_ref, iq, 124)
        )[phase]
        slots[me] = tile
        ars_ref[phase] = tile
        return send_all(peers, lambda number: ars_ref.at[phase], slots.at[me], send, recv, base)

    def ar_done(phase, copies):
        wait_all(copies)
        return jnp.sum((arx_ref, arp_ref, arq_ref)[phase][...], axis=0)

    def solve(local_sums=None, during=()):
        halves_of = [slice(0, 128), slice(128, 256)]
        to_wait = []
        for h, lanes in enumerate(halves_of):
            r1_ref[h, ix] = sd_ref[ix, 0:XR, lanes]
            to_wait.append(
                send_all(to_x, lambda g: sd_ref.at[g, 0:XR, lanes], r1_ref.at[h, ix], send, recv, 4 * h)
            )
        if during:
            during[0]()
        moved = []
        for h in range(2):
            waits(to_wait[h])
            k1_ref[h] = dot3(hx_ref, r1_ref[h].reshape(4 * XR, 128)).reshape(8, 24, 128)
            r2_ref[h, ip] = k1_ref[h, ip]
            moved.append(
                send_all(to_p, lambda s: k1_ref.at[h, s], r2_ref.at[h, ip], send, recv, 8 + 8 * h)
            )
        if during:
            during[1]()
        to_wait += moved
        for h in range(2):
            waits(moved[h])
            for y in range(4 * h, min(4 * h + 4, 7)):
                for side in range(2):
                    x2_ref[24 * y : 24 * y + 24, 128 * side : 128 * side + 128] = lane_pick(
                        [(r2_ref[h, 4 * side + s], 32 * (s - y)) for s in range(4)], 32
                    )
        k2 = dot3((hp_ref[0, 0:M, :], hp_ref[1, 0:M, :]), x2_ref[...], ((1,), (1,)))
        lane = lax.broadcasted_iota(jnp.int32, (32, 128), 1)
        rest = jnp.zeros((32, 128), F32)
        for y in range(7):
            block = lane_pick([(k2[32 * k : 32 * k + 32, :], 24 * (k - y)) for k in range(6)], 24)
            m_ref[comb(y), :] = block[:, 0:128]
            rest = jnp.where((lane >= 16 * y) & (lane < 16 * y + 16), turn(block[:, 128:256], 16 * y), rest)
        m_ref[comb(7), :] = rest
        r3_ref[rows8(8 * mine), :] = m_ref[rows8(8 * mine), :]
        copies = send_all(
            to_xq, lambda n: m_ref.at[rows8(8 * n)], r3_ref.at[rows8(8 * mine)], send, recv, 24
        )
        to_wait.append(copies)
        waits(copies)
        rest = r3_ref[comb(7), :]
        for y in range(7):
            r3x_ref[comb(y), :] = jnp.where(lane < 16, turn(rest, -16 * y), 0.0)
        k3 = dot3(hq_ref, jnp.concatenate([r3_ref[...], r3x_ref[...]], axis=1))
        energy_density = k3 * k3 * green_ref[...]
        k3 = k3 * green_ref[...]
        z3 = dot3(hqt_ref, k3)
        z3_ref[...], z3x_ref[...] = z3[:, 0:128], z3[:, 128:256]
        rest = jnp.zeros((32, 128), F32)
        for y in range(7):
            inside = (lane >= 16 * y) & (lane < 16 * y + 16)
            rest = jnp.where(inside, turn(z3x_ref[comb(y), :], 16 * y), rest)
        z3_ref[comb(7), :] = rest
        r3b_ref[rows8(8 * mine), :] = z3_ref[rows8(8 * mine), :]
        copies = send_all(
            to_xq, lambda n: z3_ref.at[rows8(8 * n)], r3b_ref.at[rows8(8 * mine)], send, recv, 56
        )
        if local_sums is not None:
            sums = ar_start(0, pack(local_sums(total(energy_density))))
        to_wait.append(copies)
        waits(copies)
        rest = r3b_ref[comb(7), :]
        loaded = [
            jnp.concatenate([r3b_ref[comb(y), :], turn(rest, -16 * y)], axis=1) for y in range(7)
        ]
        for k in range(6):
            k3b_ref[32 * k : 32 * k + 32, :] = lane_pick(
                [(loaded[y], 24 * (y - k)) for y in range(7)], 24
            )
        turned = jnp.transpose(k3b_ref[...])
        high, low = split(turned)
        v2 = dot(high, hp_ref[0]) + (dot(low, hp_ref[0]) + dot(high, hp_ref[1]))
        moved = []
        for h in range(2):
            for s in range(8):
                lanes = halves_of[s // 4]
                m2b_ref[h, s] = lane_pick(
                    [(v2[24 * y : 24 * y + 24, lanes], 32 * (y - s)) for y in range(4 * h, min(4 * h + 4, 7))],
                    32,
                )
            r2b_ref[h, ip] = m2b_ref[h, ip]
            moved.append(
                send_all(to_p, lambda s: m2b_ref.at[h, s], r2b_ref.at[h, ip], send, recv, 88 + 8 * h)
            )
        if local_sums is not None:
            sums = ar_start(1, ar_done(0, sums))
        to_wait += moved
        back = []
        for h in range(2):
            waits(moved[h])
            v1_ref[h] = dot3(hxt_ref, r2b_ref[h].reshape(M, 128)).reshape(4, XR, 128)
            r1b_ref[h, ix, 0:XR, :] = v1_ref[h, ix]
            back.append(
                send_all(to_x, lambda g: v1_ref.at[h, g], r1b_ref.at[h, ix, 0:XR], send, recv, 104 + 4 * h)
            )
        if local_sums is not None:
            sums = ar_start(2, ar_done(1, sums))
        to_wait += back
        for copies in back:
            waits(copies)
        for copies in to_wait:
            for copy in copies:
                copy.wait_send()
        return None if local_sums is None else ar_done(2, sums)

    def field(g):
        return jnp.concatenate([r1b_ref[0, g], r1b_ref[1, g]], axis=1)

    def load_field(get):
        for g in range(4):
            high, low = split(get(g))
            both = jnp.concatenate([high.astype(F32), low.astype(F32)], axis=0)
            turned = jnp.transpose(both)[0:224, :].astype(BF16)
            phi_ref[224 * g : 224 * g + 224, 0:128] = turned
            phi_ref[224 * g : 224 * g + 224, 128:256] = turned

    def x_contract(table, c, slot):
        high, low = table[c, 0:64, :], table[c, 64:128, :]
        t_ref[slot] = dot(phi_ref[...], jnp.concatenate([high, high, low, low], axis=0))

    def fold(product):
        return (product[0:8] + product[8:16]) + (product[16:24] + product[24:32])

    def in_pairs(contract, reduce):
        contract(0, 0)

        def step(i, carry):
            contract(2 * i + 1, 1)
            reduce(2 * i, 0)
            contract(2 * lax.rem(i + 1, PAIRS), 0)
            reduce(2 * i + 1, 1)
            return carry

        lax.fori_loop(0, PAIRS, step, 0)

    def sample_image(values_ref):
        def reduce(c, slot):
            m_p = mp_ref[c]
            found = jnp.zeros((8, CH), F32)
            for q in range(28):
                found = found + fold(t_ref[slot, 32 * q : 32 * q + 32, :] * m_p) * mq_ref[c, q : q + 1, :]
            image_ref[pl.ds(c, 1), :] = jnp.sum(found, axis=0, keepdims=True)

        in_pairs(lambda c, slot: x_contract(bx_ref, c, slot), reduce)
        image_ref[...] = image_ref[...] + hardness * values_ref[...]

    def sample_forces():
        def contract(c, slot):
            x_contract(bx_ref, c, slot)
            x_contract(sx_ref, c, slot + 2)

        def reduce(c, slot):
            m_p, s_p = mp_ref[c], sp_mask_ref[c]
            along_x, along_p, along_q = (jnp.zeros((8, CH), F32) for _ in range(3))
            for q in range(28):
                block = t_ref[slot, 32 * q : 32 * q + 32, :]
                m_q = mq_ref[c, q : q + 1, :]
                along_q = along_q + fold(block * m_p) * sq_mask_ref[c, q : q + 1, :]
                along_p = along_p + fold(block * s_p) * m_q
                along_x = along_x + fold(t_ref[slot + 2, 32 * q : 32 * q + 32, :] * m_p) * m_q
            minus = -charges_ref[pl.ds(c, 1), :]
            for d, along in ((0, along_x), (P_DIM, along_p), (Q_DIM, along_q)):
                out_forces_ref[d : d + 1, part(c)] = minus * jnp.sum(along, axis=0, keepdims=True)

        in_pairs(contract, reduce)

    atoms = float(ATOMS * 256)
    clear(256)
    lax.fori_loop(0, ATOMS // WIDE, net_chi, 0)
    chi = chi_ref[...]
    local_sum = total(chi)
    shift = local_sum * (1.0 / ATOMS)
    pl.semaphore_wait(barrier, len(to_xq) + len(to_p))
    copies = ar_start(0, pack([local_sum]))
    build(0, a0_ref, 0, b0_ref, chi_ref, shift)
    spread_first(0, 2)
    copies = ar_start(1, ar_done(0, copies))
    spread_first(2, 6)
    copies = ar_start(2, ar_done(1, copies))
    spread_first(6, PAIRS)
    mean = ar_done(2, copies)[0:1, 0:1] * (1.0 / atoms)
    for g in range(4):
        turned = jnp.transpose(acc_ref[256 * g : 256 * g + 256, :])
        ones = turned[128:192] + turned[192:256]
        ones_ref[g] = ones
        density = (mean - shift) * ones - (turned[0:64] + turned[64:128])
        sp_ref[g] = density
        sd_ref[g] = density
    p0 = mean - chi
    p0_ref[...] = p0
    solve(
        during=(
            lambda: lax.fori_loop(0, ATOMS // WIDE, net_short, 0),
            lambda: lax.fori_loop(0, NCH, slope_masks, 0),
        )
    )
    for g in range(4):
        phi0_ref[g] = field(g)
    load_field(field)
    sample_image(p0_ref)

    image = image_ref[...]
    image_sum = total(image)
    shift2 = image_sum * (1.0 / ATOMS)
    sums = pack([total(p0 * p0), total(p0 * image), image_sum, total(image * image), total(p0)])
    clear(128)
    copies = ar_start(0, sums)
    spread_image(0, 2)
    copies = ar_start(1, ar_done(0, copies))
    spread_image(2, 6)
    copies = ar_start(2, ar_done(1, copies))
    spread_image(6, PAIRS)
    sums = ar_done(2, copies)
    norm0, curve0, image_total, image_square, p0_total = (sums[0:1, k : k + 1] for k in range(5))
    alpha0 = norm0 / curve0
    image_mean = image_total * (1.0 / atoms)
    norm1 = (
        norm0
        - 2.0 * alpha0 * (curve0 - image_mean * p0_total)
        + alpha0 * alpha0 * (image_square - image_mean * image_total)
    )
    beta = norm1 / norm0
    residual = p0 - alpha0 * (image - image_mean)
    d1_ref[...] = residual + beta * p0
    for g in range(4):
        turned = jnp.transpose(acc_ref[256 * g : 256 * g + 256, 0:128])
        sd_ref[g] = (
            (1.0 + beta) * sp_ref[g]
            + (alpha0 * (image_mean - shift2)) * ones_ref[g]
            - alpha0 * (turned[0:64] + turned[64:128])
        )
    d1 = d1_ref[...]
    sums = solve(lambda energy: [total(residual * residual), total(hardness * d1 * d1) + energy])
    d1 = d1_ref[...]
    alpha1 = sums[0:1, 0:1] / sums[0:1, 1:2]
    charges_ref[...] = alpha0 * p0_ref[...] + alpha1 * d1
    lax.fori_loop(0, ATOMS // WIDE, net_end, 0)
    load_field(lambda g: alpha0 * phi0_ref[g] + alpha1 * field(g))
    sample_forces()


def per_device(
    descriptors, types, offsets, stencil_base, w_first, w_second, w_out, hardness,
    sr_first, sr_charge, sr_out,
):
    tabs = tables()
    vmem = pl.BlockSpec(memory_space=pltpu.VMEM)
    smem = pl.BlockSpec(memory_space=pltpu.SMEM)

    def held(*shape, dtype=F32):
        return pltpu.VMEM(shape, dtype)

    charges, forces, short_energy = pl.pallas_call(
        kernel,
        out_shape=(
            jax.ShapeDtypeStruct((ATOMS // 128, 128), F32),
            jax.ShapeDtypeStruct((3, ATOMS), F32),
            jax.ShapeDtypeStruct((ATOMS // 128, 128), F32),
        ),
        in_specs=[vmem] * 4 + [smem] + [vmem] * 12,
        out_specs=(vmem, vmem, vmem),
        scratch_shapes=[
            held(3, 5, NCH, CH), held(3, 5, NCH, CH),
            held(NCH, 64, CH), held(NCH, 32, CH), held(NCH, 32, CH),
            held(NCH, 128, CH, dtype=BF16), held(NCH, 128, CH, dtype=BF16),
            held(NCH, 32, CH), held(NCH, 32, CH),
            held(PAIRS, 1792, CH, dtype=BF16), held(PAIRS, 1792, CH, dtype=BF16),
            held(256, CH, dtype=BF16), held(256, CH, dtype=BF16),
            held(1024, 256),
            held(4, 64, LN), held(4, 64, LN), held(4, 64, LN),
            held(2, 4, XR, 128), held(2, 8, 24, 128), held(2, 8, 24, 128),
            held(256, LN), held(256, 128), held(256, 128), held(256, 128), held(M, LN),
            held(256, 128), held(256, 128), held(256, 128), held(256, LN),
            held(2, 8, 24, 128), held(2, 8, 24, 128), held(2, 4, XR, 128),
            held(2, 4, 64, 128), held(4, 64, LN), held(896, 256, dtype=BF16),
            held(NCH, CH), held(NCH, CH), held(NCH, CH),
            held(4, 896, CH),
            held(4, 8, 128), held(8, 8, 128), held(8, 8, 128), held(3, 8, 128),
            held(NCH, CH, dtype=jnp.int32), held(3, NCH, CH), held(3, NCH, CH, dtype=jnp.int32),
            held(NCH, CH), held(NCH, CH), held(32, ATOMS),
            held(192, 64), held(96, 32), held(16, 32), held(128, 128),
            pltpu.SemaphoreType.DMA((132,)),
            pltpu.SemaphoreType.DMA((132,)),
        ],
        compiler_params=pltpu.CompilerParams(
            collective_id=0, has_side_effects=True, vmem_limit_bytes=63 * 1024 * 1024
        ),
        name="equilibrate",
    )(
        descriptors, types.reshape(1, ATOMS), offsets, stencil_base, hardness,
        w_first, w_second, w_out, sr_first, sr_charge, sr_out,
        *[jnp.asarray(t) for t in tabs],
    )
    return charges.reshape(ATOMS), forces, short_energy.reshape(ATOMS)


def solution(mesh):
    rows, columns = P(AXES), P(None, AXES)
    return jax.shard_map(
        per_device,
        mesh=mesh,
        in_specs=(columns, rows, columns, columns) + (P(),) * 7,
        out_specs=(rows, columns, rows),
        check_vma=False,
    )
```

```python
import functools
import math

import jax
import jax.numpy as jnp
import numpy as np
from jax import lax
from jax.experimental import pallas as pl
from jax.experimental.pallas import tpu as pltpu
from jax.sharding import PartitionSpec as P

M = 192
SMEAR = 0.75
GX, PAX, QAX = "gx", "gz", "gy"
P_DIM, Q_DIM = 2, 1
AXES = ("gx", "gy", "gz")
ATOMS = 8192
CH = 512
NCH = ATOMS // CH
PAIRS = NCH // 2
WIDE = 2048
XR = 56
LN = 256
F32, BF16 = jnp.float32, jnp.bfloat16
MESH = pl.DeviceIdType.MESH


def cas(rows, columns):
    angle = 2.0 * np.pi * ((rows[:, None] * columns[None, :]) % M) / M
    return np.cos(angle) + np.sin(angle)


def halves(array):
    array = np.asarray(array, np.float32)
    high = array.astype(jnp.bfloat16)
    low = (array - high.astype(np.float32)).astype(jnp.bfloat16)
    return np.stack([high, low])


def tables():
    freq = np.arange(M)
    cell_x = (48 * np.arange(4)[:, None] + np.arange(XR)[None, :] - 2).reshape(-1) % M
    real_x = np.tile(np.arange(XR) < 52, 4)
    h_x = cas(freq, cell_x) * real_x[None, :]
    cell_p = (24 * np.arange(8)[:, None] + np.arange(32)[None, :] - 2).reshape(-1) % M
    real_p = np.tile(np.arange(32) < 28, 8)
    row_p = np.arange(M)
    freq_p = (row_p % 32) * 6 + row_p // 32
    h_p = np.zeros((256, 256))
    h_p[:M] = cas(freq_p, cell_p) * real_p[None, :]
    src = np.arange(256) // 8
    part = np.arange(256) % 8
    cell_q = (24 * (src % 8) + 7 * (src // 8) + part - 2) % M
    h_q = cas(freq, cell_q) * (part < 7)[None, :]
    lanes = np.zeros((8, 256), np.float32)
    lanes[0, :144] = np.arange(144) // 24
    lanes[1, :144] = np.arange(144) % 24
    return halves(h_x), halves(h_x.T), halves(h_p), halves(h_q), halves(h_q.T), lanes


def split(value):
    high = value.astype(BF16)
    return high, (value - high.astype(F32)).astype(BF16)


def dot(left, right, dims=((1,), (0,))):
    return lax.dot_general(left, right, (dims, ((), ())), preferred_element_type=F32)


def dot3(table, value, dims=((1,), (0,))):
    high, low = split(value)
    return dot(table[0], high, dims) + (dot(table[0], low, dims) + dot(table[1], high, dims))


def signed(number):
    return jnp.where(2.0 * number >= M, number - M, number)


def peers_x(ix):
    return [(step, {GX: lax.rem(ix + step, 4)}, lax.rem(ix + step, 4)) for step in (2, 1, 3)]


def peers_p(ip):
    return [(step, {PAX: lax.rem(ip + step, 8)}, lax.rem(ip + step, 8)) for step in (4, 3, 5, 2, 6, 1, 7)]


def peers_xq(ix, iq):
    steps = sorted(
        [(a, b) for a in range(4) for b in range(8) if a or b],
        key=lambda t: -(min(t[0], 4 - t[0]) + min(t[1], 8 - t[1])),
    )
    found = []
    for a, b in steps:
        g, h = lax.rem(ix + a, 4), lax.rem(iq + b, 8)
        found.append((a * 8 + b, {GX: g, QAX: h}, g * 8 + h))
    return found


def send_all(peers, src_of, dst, send, recv, base):
    copies = []
    for step, where, number in peers:
        copy = pltpu.make_async_remote_copy(
            src_ref=src_of(number),
            dst_ref=dst,
            send_sem=send.at[base + step],
            recv_sem=recv.at[base + step],
            device_id=where,
            device_id_type=MESH,
        )
        copy.start()
        copies.append(copy)
    return copies


def wait_all(copies):
    for copy in copies:
        copy.wait_recv()
    for copy in copies:
        copy.wait_send()


def rows8(start):
    return pl.ds(pl.multiple_of(start, 8), 8)


def comb(row):
    return pl.ds(row, 32, stride=8)


def turn(value, shift):
    shift = shift % value.shape[1]
    return value if shift == 0 else pltpu.roll(value, shift, 1)


def waits(copies):
    for copy in copies:
        copy.wait_recv()


def lane_pick(pieces, width):
    lane = lax.broadcasted_iota(jnp.int32, pieces[0][0].shape, 1)
    result = jnp.zeros(pieces[0][0].shape, F32)
    for number, (array, shift) in enumerate(pieces):
        inside = (lane >= number * width) & (lane < (number + 1) * width)
        result = jnp.where(inside, turn(array, shift), result)
    return result


def kernel(
    desc_hbm, types1_ref, offs1_ref, base1_ref, hard_ref,
    wf_ref, ws_ref, wo_ref, sf_ref, sc_ref, so_ref,
    hx_hbm, hxt_hbm, hp_hbm, hq_hbm, hqt_hbm, lanes_ref,
    out_charges_ref, out_forces_ref, out_short_ref,
    w_ref, s_ref, mx_ref, mp_ref, mq_ref, bx_ref, sx_ref, sp_mask_ref, sq_mask_ref,
    a0_ref, a1_ref, b0_ref, b1_ref, acc_ref,
    ones_ref, sp_ref, sd_ref, r1_ref, k1_ref, r2_ref, x2_ref, m_ref, r3_ref, r3x_ref, green_ref,
    z3_ref, z3x_ref, r3b_ref, k3b_ref, m2b_ref, r2b_ref, v1_ref, r1b_ref, phi0_ref, phi_ref,
    image_ref, p0_ref, d1_ref, t_ref, arp_ref, arq_ref, ars_ref,
    types_ref, offs_ref, base_ref, chi_ref, charges_ref, pre_ref, n1_ref, n2_ref, n3_ref, tall_ref,
    alpha_ref, first_ref, second_ref, last_ref, desc_ref, hx_ref, hxt_ref, hp_ref, hq_ref, hqt_ref, load,
    send, recv,
):
    ix, ip, iq = lax.axis_index(GX), lax.axis_index(PAX), lax.axis_index(QAX)
    mine = ix * 8 + iq
    to_x, to_p, to_xq = peers_x(ix), peers_p(ip), peers_xq(ix, iq)
    loads = [
        pltpu.make_async_copy(source, target, load.at[k])
        for k, (source, target) in enumerate(
            (
                (desc_hbm, desc_ref), (hx_hbm, hx_ref), (hp_hbm, hp_ref), (hq_hbm, hq_ref),
                (hqt_hbm, hqt_ref), (hxt_hbm, hxt_ref),
            )
        )
    ]
    for copy in loads:
        copy.start()
    barrier = pltpu.get_barrier_semaphore()
    for _, where, _ in to_xq + to_p:
        pl.semaphore_signal(barrier, inc=1, device_id=where, device_id_type=MESH)

    def part(c):
        return pl.ds(c * CH, CH)

    for c in range(NCH):
        types_ref[c : c + 1, :] = types1_ref[:, c * CH : c * CH + CH]
        for d in range(3):
            offs_ref[d, c : c + 1, :] = offs1_ref[d : d + 1, c * CH : c * CH + CH]
            base_ref[d, c : c + 1, :] = base1_ref[d : d + 1, c * CH : c * CH + CH]

    n1_ref[...] = jnp.zeros(n1_ref.shape, F32)
    n2_ref[...] = jnp.zeros(n2_ref.shape, F32)
    n3_ref[...] = jnp.zeros(n3_ref.shape, F32)
    tall_ref[...] = jnp.zeros(tall_ref.shape, F32)
    for e in range(3):
        n1_ref[32 * e : 32 * e + 25, 0:64] = wf_ref[e]
        n1_ref[96 + 32 * e : 96 + 32 * e + 25, 0:64] = sf_ref[e]
        n2_ref[32 * e : 32 * e + 25, 0:25] = ws_ref[e]
    n3_ref[0:3, 0:25] = wo_ref[...]
    n3_ref[16:19, 0:25] = so_ref[...]
    tall_ref[0:3, 0:25] = sc_ref[...]
    tall_ref[...] = jnp.transpose(tall_ref[...])
    high, low = split(n1_ref[...])
    high = high.astype(F32)
    first_ref[:, 0:128] = (high + pltpu.roll(high, 64, 1)).astype(BF16)
    first_ref[:, 128:256] = low
    for source, stacked in ((n2_ref, second_ref), (n3_ref, last_ref)):
        high, low = (half.astype(F32) for half in split(source[...]))
        stacked[...] = (high + pltpu.roll(high, 32, 1) + pltpu.roll(low, 64, 1)).astype(BF16)

    def layer(weights, value):
        high, low = split(value)
        return dot(weights, jnp.concatenate([high, low, high], axis=0))

    def wide(i):
        return pl.ds(i * WIDE, WIDE)

    def by_type(i, first, second, third):
        kind = types1_ref[:, wide(i)]
        return jnp.where(kind == 0, first, jnp.where(kind == 1, second, third))

    def net_chi(i, carry):
        pre = layer(first_ref[0:96, 0:192], desc_ref[:, wide(i)])
        hidden = jnp.tanh(by_type(i, pre[0:32], pre[32:64], pre[64:96]))
        pre = layer(second_ref[:, 0:96], hidden)
        hidden = jnp.tanh(by_type(i, pre[0:32], pre[32:64], pre[64:96]))
        value = layer(last_ref[0:16, 0:96], hidden)
        value = by_type(i, value[0:1], value[1:2], value[2:3])
        for k in range(WIDE // CH):
            chi_ref[pl.ds(WIDE // CH * i + k, 1), :] = value[:, CH * k : CH * k + CH]
        return carry

    def net_short(i, carry):
        pre = layer(first_ref[96:192, 0:192], desc_ref[:, wide(i)])
        pre_ref[:, wide(i)] = by_type(i, pre[0:32], pre[32:64], pre[64:96])
        return carry

    def net_end(i, carry):
        rows = [charges_ref[pl.ds(WIDE // CH * i + k, 1), :] for k in range(WIDE // CH)]
        charge = jnp.concatenate(rows, axis=1)
        weight = by_type(i, tall_ref[0:32, 0:1], tall_ref[0:32, 1:2], tall_ref[0:32, 2:3])
        hidden = jnp.tanh(pre_ref[:, wide(i)] + weight * charge)
        value = layer(last_ref[16:32, 0:96], hidden)
        value = by_type(i, value[0:1], value[1:2], value[2:3])
        for k in range(WIDE // 128):
            row = pl.ds(WIDE // 128 * i + k, 1)
            out_short_ref[row, :] = value[:, 128 * k : 128 * k + 128]
            out_charges_ref[row, :] = charge[:, 128 * k : 128 * k + 128]
        return carry

    hardness = jnp.where(
        types_ref[...] == 0, hard_ref[0], jnp.where(types_ref[...] == 1, hard_ref[1], hard_ref[2])
    )
    for d in range(3):
        t = offs_ref[d]
        spline = [t, 1.0 - t]
        for order in (3, 4, 5):
            grown = []
            for k in range(order):
                term = None
                if k < order - 1:
                    term = (t + k) * spline[k]
                if k >= 1:
                    other = (order - k - t) * spline[k - 1]
                    term = other if term is None else term + other
                grown.append(term * (1.0 / (order - 1)))
            if order == 5:
                s_ref[d, 0] = -spline[3]
                s_ref[d, 1] = spline[3] - spline[2]
                s_ref[d, 2] = spline[2] - spline[1]
                s_ref[d, 3] = spline[1] - spline[0]
                s_ref[d, 4] = spline[0]
            spline = grown
        for j in range(5):
            w_ref[d, j] = spline[4 - j]

    row = lax.broadcasted_iota(jnp.int32, (M, LN), 0).astype(F32)
    f_q = signed(row)
    f_p = signed(lanes_ref[0:1, :] + (6 * mine).astype(F32))
    f_x = signed(lanes_ref[1:2, :] + (24 * ip).astype(F32))
    factor = 2.0 * math.pi / M
    wave = (factor * factor) * (f_q * f_q + (f_p * f_p + f_x * f_x))
    safe = jnp.where(wave > 0, wave, 1.0)
    green_ref[...] = jnp.where(
        wave > 0, (4.0 * math.pi / (M * M * M)) * jnp.exp((-0.5 * SMEAR * SMEAR) * wave) / safe, 0.0
    )

    for g in range(4):
        for h in range(2):
            r1b_ref[h, g, XR : XR + 8, :] = jnp.zeros((8, 128), F32)
        acc_ref[256 * g + 224 : 256 * g + 256, :] = jnp.zeros((32, 256), F32)
    x2_ref[168:256, :] = jnp.zeros((88, LN), F32)
    r3x_ref[comb(7), :] = jnp.zeros((32, 128), F32)
    k3b_ref[192:256, :] = jnp.zeros((64, LN), F32)

    def mask(table, d, c, count):
        base = base_ref[d, pl.ds(c, 1), :]
        place = lax.broadcasted_iota(jnp.int32, (count, CH), 0) - base
        result = jnp.zeros((count, CH), F32)
        for j in range(5):
            result = jnp.where(place == j, table[d, j, pl.ds(c, 1), :], result)
        return result

    def slope_masks(c, carry):
        high, low = split(mask(s_ref, 0, c, 64))
        sx_ref[c, 0:64, :], sx_ref[c, 64:128, :] = high, low
        sp_mask_ref[c], sq_mask_ref[c] = mask(s_ref, P_DIM, c, 32), mask(s_ref, Q_DIM, c, 32)
        return carry

    def build(c, a_ref, i, b_ref, values_ref, shift):
        m_x, m_p, m_q = mask(w_ref, 0, c, 64), mask(w_ref, P_DIM, c, 32), mask(w_ref, Q_DIM, c, 32)
        mx_ref[c], mp_ref[c], mq_ref[c] = m_x, m_p, m_q
        for q in range(28):
            high, low = split(m_p * m_q[q : q + 1, :])
            a_ref[i, 32 * q : 32 * q + 32, :] = high
            a_ref[i, 896 + 32 * q : 896 + 32 * q + 32, :] = low
        high, low = split(m_x)
        b_ref[128:192, :], b_ref[192:256, :] = high, low
        bx_ref[c, 0:64, :], bx_ref[c, 64:128, :] = high, low
        b_ref[0:64, :], b_ref[64:128, :] = split(m_x * (values_ref[pl.ds(c, 1), :] - shift))

    def gather_part(part, width):
        for g in range(4):
            acc_ref[256 * g : 256 * g + 224, 0:width] += (
                part[224 * g : 224 * g + 224] + part[896 + 224 * g : 896 + 224 * g + 224]
            )

    def spread_first(lo, hi):
        def step(i, carry):
            part = dot(a0_ref[i], b0_ref[...], ((1,), (1,)))
            build(2 * i + 1, a1_ref, i, b1_ref, chi_ref, shift)
            gather_part(part, 256)
            part = dot(a1_ref[i], b1_ref[...], ((1,), (1,)))
            after = lax.rem(i + 1, PAIRS)
            build(2 * after, a0_ref, after, b0_ref, chi_ref, shift)
            gather_part(part, 256)
            return carry

        lax.fori_loop(lo, hi, step, 0)

    def spread_image(lo, hi):
        def step(i, carry):
            for c, b_ref in ((2 * i, b0_ref), (2 * i + 1, b1_ref)):
                value = image_ref[pl.ds(c, 1), :] - shift2
                b_ref[0:64, :], b_ref[64:128, :] = split(mx_ref[c] * value)
            part = dot(a0_ref[i], b0_ref[0:128, :], ((1,), (1,)))
            other = dot(a1_ref[i], b1_ref[0:128, :], ((1,), (1,)))
            gather_part(part, 128)
            gather_part(other, 128)
            return carry

        lax.fori_loop(lo, hi, step, 0)

    def clear(width):
        for g in range(4):
            acc_ref[256 * g : 256 * g + 224, 0:width] = jnp.zeros((224, width), F32)

    lane = lax.broadcasted_iota(jnp.int32, (8, 128), 1)

    def pack(sums):
        tile = jnp.zeros((8, 128), F32)
        for k, value in enumerate(sums):
            tile = jnp.where(lane == k, value, tile)
        return tile

    def total(array):
        return jnp.sum(jnp.sum(array, axis=0, keepdims=True), axis=1, keepdims=True)

    def ar_start(phase, tile):
        peers, slots, me, base = ((to_p, arp_ref, ip, 112), (to_xq, arq_ref, mine, 120))[phase]
        slots[me] = tile
        ars_ref[phase] = tile
        return send_all(peers, lambda number: ars_ref.at[phase], slots.at[me], send, recv, base)

    def ar_done(phase, copies):
        wait_all(copies)
        return jnp.sum((arp_ref, arq_ref)[phase][...], axis=0)

    def solve(local_sums=None, during=(), finish=None):
        halves_of = [slice(0, 128), slice(128, 256)]
        to_wait = []
        for h, lanes in enumerate(halves_of):
            r1_ref[h, ix] = sd_ref[ix, 0:XR, lanes]
            to_wait.append(
                send_all(to_x, lambda g: sd_ref.at[g, 0:XR, lanes], r1_ref.at[h, ix], send, recv, 4 * h)
            )
        if during:
            during[0]()
        moved = []
        for h in range(2):
            waits(to_wait[h])
            k1_ref[h] = dot3(hx_ref, r1_ref[h].reshape(4 * XR, 128)).reshape(8, 24, 128)
            r2_ref[h, ip] = k1_ref[h, ip]
            moved.append(
                send_all(to_p, lambda s: k1_ref.at[h, s], r2_ref.at[h, ip], send, recv, 8 + 8 * h)
            )
        if during:
            during[1]()
        to_wait += moved
        for h in range(2):
            waits(moved[h])
            for y in range(4 * h, min(4 * h + 4, 7)):
                for side in range(2):
                    x2_ref[24 * y : 24 * y + 24, 128 * side : 128 * side + 128] = lane_pick(
                        [(r2_ref[h, 4 * side + s], 32 * (s - y)) for s in range(4)], 32
                    )
        k2 = dot3((hp_ref[0, 0:M, :], hp_ref[1, 0:M, :]), x2_ref[...], ((1,), (1,)))
        lane = lax.broadcasted_iota(jnp.int32, (32, 128), 1)
        rest = jnp.zeros((32, 128), F32)
        for y in range(7):
            block = lane_pick([(k2[32 * k : 32 * k + 32, :], 24 * (k - y)) for k in range(6)], 24)
            m_ref[comb(y), :] = block[:, 0:128]
            rest = jnp.where((lane >= 16 * y) & (lane < 16 * y + 16), turn(block[:, 128:256], 16 * y), rest)
        m_ref[comb(7), :] = rest
        r3_ref[rows8(8 * mine), :] = m_ref[rows8(8 * mine), :]
        copies = send_all(
            to_xq, lambda n: m_ref.at[rows8(8 * n)], r3_ref.at[rows8(8 * mine)], send, recv, 24
        )
        to_wait.append(copies)
        waits(copies)
        rest = r3_ref[comb(7), :]
        for y in range(7):
            r3x_ref[comb(y), :] = jnp.where(lane < 16, turn(rest, -16 * y), 0.0)
        k3 = dot3(hq_ref, jnp.concatenate([r3_ref[...], r3x_ref[...]], axis=1))
        energy_density = k3 * k3 * green_ref[...]
        k3 = k3 * green_ref[...]
        z3 = dot3(hqt_ref, k3)
        z3_ref[...], z3x_ref[...] = z3[:, 0:128], z3[:, 128:256]
        rest = jnp.zeros((32, 128), F32)
        for y in range(7):
            inside = (lane >= 16 * y) & (lane < 16 * y + 16)
            rest = jnp.where(inside, turn(z3x_ref[comb(y), :], 16 * y), rest)
        z3_ref[comb(7), :] = rest
        r3b_ref[rows8(8 * mine), :] = z3_ref[rows8(8 * mine), :]
        copies = send_all(
            to_xq, lambda n: z3_ref.at[rows8(8 * n)], r3b_ref.at[rows8(8 * mine)], send, recv, 56
        )
        if local_sums is not None:
            sums = ar_start(0, pack(local_sums(total(energy_density))))
        to_wait.append(copies)
        waits(copies)
        if local_sums is not None:
            sums = ar_start(1, ar_done(0, sums))
        rest = r3b_ref[comb(7), :]
        loaded = [
            jnp.concatenate([r3b_ref[comb(y), :], turn(rest, -16 * y)], axis=1) for y in range(7)
        ]
        for k in range(6):
            k3b_ref[32 * k : 32 * k + 32, :] = lane_pick(
                [(loaded[y], 24 * (y - k)) for y in range(7)], 24
            )
        turned = jnp.transpose(k3b_ref[...])
        high, low = split(turned)
        v2 = dot(high, hp_ref[0]) + (dot(low, hp_ref[0]) + dot(high, hp_ref[1]))
        moved = []
        for h in range(2):
            for s in range(8):
                lanes = halves_of[s // 4]
                m2b_ref[h, s] = lane_pick(
                    [(v2[24 * y : 24 * y + 24, lanes], 32 * (y - s)) for y in range(4 * h, min(4 * h + 4, 7))],
                    32,
                )
            r2b_ref[h, ip] = m2b_ref[h, ip]
            moved.append(
                send_all(to_p, lambda s: m2b_ref.at[h, s], r2b_ref.at[h, ip], send, recv, 88 + 8 * h)
            )
        to_wait += moved
        back = []
        for h in range(2):
            waits(moved[h])
            v1_ref[h] = dot3(hxt_ref, r2b_ref[h].reshape(M, 128)).reshape(4, XR, 128)
            r1b_ref[h, ix, 0:XR, :] = v1_ref[h, ix]
            back.append(
                send_all(to_x, lambda g: v1_ref.at[h, g], r1b_ref.at[h, ix, 0:XR], send, recv, 104 + 4 * h)
            )
        to_wait += back
        if finish is not None:
            finish(ar_done(1, sums))
        for copies in back:
            waits(copies)
        for copies in to_wait:
            for copy in copies:
                copy.wait_send()

    def field(g):
        return jnp.concatenate([r1b_ref[0, g], r1b_ref[1, g]], axis=1)

    def load_field(get):
        for g in range(4):
            high, low = split(get(g))
            both = jnp.concatenate([high.astype(F32), low.astype(F32)], axis=0)
            turned = jnp.transpose(both)[0:224, :].astype(BF16)
            phi_ref[224 * g : 224 * g + 224, 0:128] = turned
            phi_ref[224 * g : 224 * g + 224, 128:192] = turned[:, 0:64]

    def x_contract(table, c, slot):
        high, low = table[c, 0:64, :], table[c, 64:128, :]
        t_ref[slot] = dot(phi_ref[...], jnp.concatenate([high, high, low], axis=0))

    def fold(product):
        return (product[0:8] + product[8:16]) + (product[16:24] + product[24:32])

    def in_pairs(contract, reduce):
        contract(0, 0)

        def step(i, carry):
            contract(2 * i + 1, 1)
            reduce(2 * i, 0)
            contract(2 * lax.rem(i + 1, PAIRS), 0)
            reduce(2 * i + 1, 1)
            return carry

        lax.fori_loop(0, PAIRS, step, 0)

    def sample_image(values_ref):
        def reduce(c, slot):
            m_p = mp_ref[c]
            found = jnp.zeros((8, CH), F32)
            for q in range(28):
                found = found + fold(t_ref[slot, 32 * q : 32 * q + 32, :] * m_p) * mq_ref[c, q : q + 1, :]
            image_ref[pl.ds(c, 1), :] = jnp.sum(found, axis=0, keepdims=True)

        in_pairs(lambda c, slot: x_contract(bx_ref, c, slot), reduce)
        image_ref[...] = image_ref[...] + hardness * values_ref[...]

    def sample_forces():
        def contract(c, slot):
            x_contract(bx_ref, c, slot)
            x_contract(sx_ref, c, slot + 2)

        def reduce(c, slot):
            m_p, s_p = mp_ref[c], sp_mask_ref[c]
            along_x, along_p, along_q = (jnp.zeros((8, CH), F32) for _ in range(3))
            for q in range(28):
                block = t_ref[slot, 32 * q : 32 * q + 32, :]
                m_q = mq_ref[c, q : q + 1, :]
                along_q = along_q + fold(block * m_p) * sq_mask_ref[c, q : q + 1, :]
                along_p = along_p + fold(block * s_p) * m_q
                along_x = along_x + fold(t_ref[slot + 2, 32 * q : 32 * q + 32, :] * m_p) * m_q
            minus = -charges_ref[pl.ds(c, 1), :]
            for d, along in ((0, along_x), (P_DIM, along_p), (Q_DIM, along_q)):
                out_forces_ref[d : d + 1, part(c)] = minus * jnp.sum(along, axis=0, keepdims=True)

        in_pairs(contract, reduce)

    atoms = float(ATOMS * 256)
    clear(256)
    loads[0].wait()
    lax.fori_loop(0, ATOMS // WIDE, net_chi, 0)
    chi = chi_ref[...]
    local_sum = total(chi)
    shift = local_sum * (1.0 / ATOMS)
    build(0, a0_ref, 0, b0_ref, chi_ref, shift)
    spread_first(0, 2)
    pl.semaphore_wait(barrier, len(to_xq) + len(to_p))
    copies = ar_start(0, pack([local_sum]))
    spread_first(2, 4)
    copies = ar_start(1, ar_done(0, copies))
    spread_first(4, PAIRS)
    mean = ar_done(1, copies)[0:1, 0:1] * (1.0 / atoms)
    for g in range(4):
        turned = jnp.transpose(acc_ref[256 * g : 256 * g + 256, :])
        ones = turned[128:192] + turned[192:256]
        ones_ref[g] = ones
        density = (mean - shift) * ones - (turned[0:64] + turned[64:128])
        sp_ref[g] = density
        sd_ref[g] = density
    p0 = mean - chi
    p0_ref[...] = p0
    for copy in loads[1:]:
        copy.wait()
    solve(
        during=(
            lambda: lax.fori_loop(0, ATOMS // WIDE, net_short, 0),
            lambda: lax.fori_loop(0, NCH, slope_masks, 0),
        )
    )
    for g in range(4):
        phi0_ref[g] = field(g)
    load_field(field)
    sample_image(p0_ref)

    image = image_ref[...]
    image_sum = total(image)
    shift2 = image_sum * (1.0 / ATOMS)
    sums = pack([total(p0 * p0), total(p0 * image), image_sum, total(image * image), total(p0)])
    clear(128)
    copies = ar_start(0, sums)
    spread_image(0, 3)
    copies = ar_start(1, ar_done(0, copies))
    spread_image(3, PAIRS)
    sums = ar_done(1, copies)
    norm0, curve0, image_total, image_square, p0_total = (sums[0:1, k : k + 1] for k in range(5))
    alpha0 = norm0 / curve0
    image_mean = image_total * (1.0 / atoms)
    norm1 = (
        norm0
        - 2.0 * alpha0 * (curve0 - image_mean * p0_total)
        + alpha0 * alpha0 * (image_square - image_mean * image_total)
    )
    beta = norm1 / norm0
    residual = p0 - alpha0 * (image - image_mean)
    d1_ref[...] = residual + beta * p0
    for g in range(4):
        turned = jnp.transpose(acc_ref[256 * g : 256 * g + 256, 0:128])
        sd_ref[g] = (
            (1.0 + beta) * sp_ref[g]
            + (alpha0 * (image_mean - shift2)) * ones_ref[g]
            - alpha0 * (turned[0:64] + turned[64:128])
        )
    d1 = d1_ref[...]
    def finish(sums):
        alpha1 = sums[0:1, 0:1] / sums[0:1, 1:2]
        charges_ref[...] = alpha0 * p0_ref[...] + alpha1 * d1_ref[...]
        for g in range(4):
            phi0_ref[g] = alpha0 * phi0_ref[g]
        alpha_ref[...] = jnp.zeros((8, 128), F32) + alpha1
        lax.fori_loop(0, ATOMS // WIDE, net_end, 0)

    solve(
        lambda energy: [total(residual * residual), total(hardness * d1 * d1) + energy],
        finish=finish,
    )
    alpha1 = alpha_ref[0:1, 0:1]
    load_field(lambda g: phi0_ref[g] + alpha1 * field(g))
    sample_forces()


def hand_over(*refs):
    for source, target in zip(refs[:3], refs[3:]):
        target[...] = source[...]


def per_device(
    descriptors, types, offsets, stencil_base, w_first, w_second, w_out, hardness,
    sr_first, sr_charge, sr_out,
):
    tabs = tables()
    vmem = pl.BlockSpec(memory_space=pltpu.VMEM)
    smem = pl.BlockSpec(memory_space=pltpu.SMEM)
    far = pl.BlockSpec(memory_space=pl.ANY)

    def held(*shape, dtype=F32):
        return pltpu.VMEM(shape, dtype)

    results = pl.pallas_call(
        kernel,
        out_shape=(
            jax.ShapeDtypeStruct((ATOMS // 128, 128), F32),
            jax.ShapeDtypeStruct((3, ATOMS), F32),
            jax.ShapeDtypeStruct((ATOMS // 128, 128), F32),
        ),
        in_specs=[far] + [vmem] * 3 + [smem] + [vmem] * 6 + [far] * 5 + [vmem],
        out_specs=(vmem, vmem, vmem),
        scratch_shapes=[
            held(3, 5, NCH, CH), held(3, 5, NCH, CH),
            held(NCH, 64, CH), held(NCH, 32, CH), held(NCH, 32, CH),
            held(NCH, 128, CH, dtype=BF16), held(NCH, 128, CH, dtype=BF16),
            held(NCH, 32, CH), held(NCH, 32, CH),
            held(PAIRS, 1792, CH, dtype=BF16), held(PAIRS, 1792, CH, dtype=BF16),
            held(256, CH, dtype=BF16), held(256, CH, dtype=BF16),
            held(1024, 256),
            held(4, 64, LN), held(4, 64, LN), held(4, 64, LN),
            held(2, 4, XR, 128), held(2, 8, 24, 128), held(2, 8, 24, 128),
            held(256, LN), held(256, 128), held(256, 128), held(256, 128), held(M, LN),
            held(256, 128), held(256, 128), held(256, 128), held(256, LN),
            held(2, 8, 24, 128), held(2, 8, 24, 128), held(2, 4, XR, 128),
            held(2, 4, 64, 128), held(4, 64, LN), held(896, 192, dtype=BF16),
            held(NCH, CH), held(NCH, CH), held(NCH, CH),
            held(4, 896, CH),
            held(8, 8, 128), held(32, 8, 128), held(2, 8, 128),
            held(NCH, CH, dtype=jnp.int32), held(3, NCH, CH), held(3, NCH, CH, dtype=jnp.int32),
            held(NCH, CH), held(NCH, CH), held(32, ATOMS),
            held(192, 128), held(96, 128), held(32, 128), held(128, 128),
            held(8, 128), held(192, 256, dtype=BF16), held(96, 128, dtype=BF16), held(32, 128, dtype=BF16),
            held(64, ATOMS), held(2, M, 224, dtype=BF16), held(2, 224, M, dtype=BF16),
            held(2, 256, 256, dtype=BF16), held(2, M, 256, dtype=BF16), held(2, 256, M, dtype=BF16),
            pltpu.SemaphoreType.DMA((6,)),
            pltpu.SemaphoreType.DMA((152,)),
            pltpu.SemaphoreType.DMA((152,)),
        ],
        compiler_params=pltpu.CompilerParams(
            collective_id=0, has_side_effects=True, vmem_limit_bytes=63 * 1024 * 1024
        ),
        name="equilibrate",
    )(
        descriptors, types.reshape(1, ATOMS), offsets, stencil_base, hardness,
        w_first, w_second, w_out, sr_first, sr_charge, sr_out,
        *[jnp.asarray(t) for t in tabs],
    )
    charges, forces, short_energy = pl.pallas_call(
        hand_over,
        out_shape=tuple(jax.ShapeDtypeStruct(r.shape, F32) for r in results),
        in_specs=[vmem] * 3,
        out_specs=(vmem,) * 3,
        name="hand_over",
    )(*results)
    return charges.reshape(ATOMS), forces, short_energy.reshape(ATOMS)


def solution(mesh):
    rows, columns = P(AXES), P(None, AXES)
    return jax.shard_map(
        per_device,
        mesh=mesh,
        in_specs=(columns, rows, columns, columns) + (P(),) * 7,
        out_specs=(rows, columns, rows),
        check_vma=False,
    )
```

```python
import functools
import math

import jax
import jax.numpy as jnp
import numpy as np
from jax import lax
from jax.experimental import pallas as pl
from jax.experimental.pallas import tpu as pltpu
from jax.sharding import PartitionSpec as P

M = 192
SMEAR = 0.75
GX, PAX, QAX = "gx", "gz", "gy"
P_DIM, Q_DIM = 2, 1
AXES = ("gx", "gy", "gz")
ATOMS = 8192
CH = 512
NCH = ATOMS // CH
PAIRS = NCH // 2
WIDE = 2048
XR = 56
LN = 256
F32, BF16 = jnp.float32, jnp.bfloat16
MESH = pl.DeviceIdType.MESH


def cas(rows, columns):
    angle = 2.0 * np.pi * ((rows[:, None] * columns[None, :]) % M) / M
    return np.cos(angle) + np.sin(angle)


def halves(array):
    array = np.asarray(array, np.float32)
    high = array.astype(jnp.bfloat16)
    low = (array - high.astype(np.float32)).astype(jnp.bfloat16)
    return np.stack([high, low])


def tables():
    freq = np.arange(M)
    cell_x = (48 * np.arange(4)[:, None] + np.arange(XR)[None, :] - 2).reshape(-1) % M
    real_x = np.tile(np.arange(XR) < 52, 4)
    h_x = cas(freq, cell_x) * real_x[None, :]
    cell_p = (24 * np.arange(8)[:, None] + np.arange(32)[None, :] - 2).reshape(-1) % M
    real_p = np.tile(np.arange(32) < 28, 8)
    row_p = np.arange(M)
    freq_p = (row_p % 32) * 6 + row_p // 32
    h_p = np.zeros((256, 256))
    h_p[:M] = cas(freq_p, cell_p) * real_p[None, :]
    src = np.arange(256) // 8
    part = np.arange(256) % 8
    cell_q = (24 * (src % 8) + 7 * (src // 8) + part - 2) % M
    h_q = cas(freq, cell_q) * (part < 7)[None, :]
    lanes = np.zeros((8, 256), np.float32)
    lanes[0, :144] = np.arange(144) // 24
    lanes[1, :144] = np.arange(144) % 24
    return halves(h_x), halves(h_x.T), halves(h_p), halves(h_q), halves(h_q.T), lanes


def split(value):
    high = value.astype(BF16)
    return high, (value - high.astype(F32)).astype(BF16)


def dot(left, right, dims=((1,), (0,))):
    return lax.dot_general(left, right, (dims, ((), ())), preferred_element_type=F32)


def dot3(table, value, dims=((1,), (0,))):
    high, low = split(value)
    return dot(table[0], high, dims) + (dot(table[0], low, dims) + dot(table[1], high, dims))


def signed(number):
    return jnp.where(2.0 * number >= M, number - M, number)


def peers_x(ix):
    return [(step, {GX: lax.rem(ix + step, 4)}, lax.rem(ix + step, 4)) for step in (2, 1, 3)]


def peers_p(ip):
    return [(step, {PAX: lax.rem(ip + step, 8)}, lax.rem(ip + step, 8)) for step in (4, 3, 5, 2, 6, 1, 7)]


def peers_xq(ix, iq):
    steps = sorted(
        [(a, b) for a in range(4) for b in range(8) if a or b],
        key=lambda t: -(min(t[0], 4 - t[0]) + min(t[1], 8 - t[1])),
    )
    found = []
    for a, b in steps:
        g, h = lax.rem(ix + a, 4), lax.rem(iq + b, 8)
        found.append((a * 8 + b, {GX: g, QAX: h}, g * 8 + h))
    return found


def send_all(peers, src_of, dst, send, recv, base):
    copies = []
    for step, where, number in peers:
        copy = pltpu.make_async_remote_copy(
            src_ref=src_of(number),
            dst_ref=dst,
            send_sem=send.at[base + step],
            recv_sem=recv.at[base + step],
            device_id=where,
            device_id_type=MESH,
        )
        copy.start()
        copies.append(copy)
    return copies


def wait_all(copies):
    for copy in copies:
        copy.wait_recv()
    for copy in copies:
        copy.wait_send()


def rows8(start):
    return pl.ds(pl.multiple_of(start, 8), 8)


def comb(row):
    return pl.ds(row, 32, stride=8)


def turn(value, shift):
    shift = shift % value.shape[1]
    return value if shift == 0 else pltpu.roll(value, shift, 1)


def waits(copies):
    for copy in copies:
        copy.wait_recv()


def lane_pick(pieces, width):
    lane = lax.broadcasted_iota(jnp.int32, pieces[0][0].shape, 1)
    result = jnp.zeros(pieces[0][0].shape, F32)
    for number, (array, shift) in enumerate(pieces):
        inside = (lane >= number * width) & (lane < (number + 1) * width)
        result = jnp.where(inside, turn(array, shift), result)
    return result


def kernel(
    desc_hbm, types1_ref, offs1_ref, base1_ref, hard_ref,
    wf_ref, ws_ref, wo_ref, sf_ref, sc_ref, so_ref,
    hx_hbm, hxt_hbm, hp_hbm, hq_hbm, hqt_hbm, lanes_ref,
    out_charges_ref, out_forces_ref, out_short_ref,
    w_ref, s_ref, mx_ref, mp_ref, mq_ref, bx_ref, sx_ref, sp_mask_ref, sq_mask_ref,
    a0_ref, a1_ref, b0_ref, b1_ref, acc_ref,
    ones_ref, sp_ref, sd_ref, r1_ref, k1_ref, r2_ref, x2_ref, m_ref, r3_ref, r3x_ref, green_ref,
    z3_ref, z3x_ref, r3b_ref, k3b_ref, m2b_ref, r2b_ref, v1_ref, r1b_ref, phi0_ref, phi_ref,
    image_ref, p0_ref, d1_ref, t_ref, arp_ref, arq_ref, ars_ref,
    types_ref, offs_ref, base_ref, chi_ref, charges_ref, pre_ref, n1_ref, n2_ref, n3_ref, tall_ref,
    alpha_ref, first_ref, second_ref, last_ref, desc_ref, hx_ref, hxt_ref, hp_ref, hq_ref, hqt_ref, load,
    send, recv,
):
    ix, ip, iq = lax.axis_index(GX), lax.axis_index(PAX), lax.axis_index(QAX)
    mine = ix * 8 + iq
    to_x, to_p, to_xq = peers_x(ix), peers_p(ip), peers_xq(ix, iq)
    loads = [
        pltpu.make_async_copy(source, target, load.at[k])
        for k, (source, target) in enumerate(
            (
                (hx_hbm, hx_ref), (hp_hbm, hp_ref), (hq_hbm, hq_ref),
                (hqt_hbm, hqt_ref), (hxt_hbm, hxt_ref),
            )
        )
    ]

    def piece(i):
        lanes = pl.ds(i * WIDE, WIDE)
        return pltpu.make_async_copy(desc_hbm.at[:, lanes], desc_ref.at[:, lanes], load.at[5 + i])

    for i in range(ATOMS // WIDE):
        piece(i).start()
    barrier = pltpu.get_barrier_semaphore()
    for _, where, _ in to_xq + to_p:
        pl.semaphore_signal(barrier, inc=1, device_id=where, device_id_type=MESH)

    def part(c):
        return pl.ds(c * CH, CH)

    for c in range(NCH):
        types_ref[c : c + 1, :] = types1_ref[:, c * CH : c * CH + CH]
        for d in range(3):
            offs_ref[d, c : c + 1, :] = offs1_ref[d : d + 1, c * CH : c * CH + CH]
            base_ref[d, c : c + 1, :] = base1_ref[d : d + 1, c * CH : c * CH + CH]

    n1_ref[...] = jnp.zeros(n1_ref.shape, F32)
    n2_ref[...] = jnp.zeros(n2_ref.shape, F32)
    n3_ref[...] = jnp.zeros(n3_ref.shape, F32)
    tall_ref[...] = jnp.zeros(tall_ref.shape, F32)
    for e in range(3):
        n1_ref[32 * e : 32 * e + 25, 0:64] = wf_ref[e]
        n1_ref[96 + 32 * e : 96 + 32 * e + 25, 0:64] = sf_ref[e]
        n2_ref[32 * e : 32 * e + 25, 0:25] = ws_ref[e]
    n3_ref[0:3, 0:25] = wo_ref[...]
    n3_ref[16:19, 0:25] = so_ref[...]
    tall_ref[0:3, 0:25] = sc_ref[...]
    tall_ref[...] = jnp.transpose(tall_ref[...])
    high, low = split(n1_ref[...])
    high = high.astype(F32)
    first_ref[:, 0:128] = (high + pltpu.roll(high, 64, 1)).astype(BF16)
    first_ref[:, 128:256] = low
    for source, stacked in ((n2_ref, second_ref), (n3_ref, last_ref)):
        high, low = (half.astype(F32) for half in split(source[...]))
        stacked[...] = (high + pltpu.roll(high, 32, 1) + pltpu.roll(low, 64, 1)).astype(BF16)

    def layer(weights, value):
        high, low = split(value)
        return dot(weights, jnp.concatenate([high, low, high], axis=0))

    def wide(i):
        return pl.ds(i * WIDE, WIDE)

    def by_type(i, first, second, third):
        kind = types1_ref[:, wide(i)]
        return jnp.where(kind == 0, first, jnp.where(kind == 1, second, third))

    def net_chi(i, carry):
        piece(i).wait()
        pre = layer(first_ref[0:96, 0:192], desc_ref[:, wide(i)])
        hidden = jnp.tanh(by_type(i, pre[0:32], pre[32:64], pre[64:96]))
        pre = layer(second_ref[:, 0:96], hidden)
        hidden = jnp.tanh(by_type(i, pre[0:32], pre[32:64], pre[64:96]))
        value = layer(last_ref[0:16, 0:96], hidden)
        value = by_type(i, value[0:1], value[1:2], value[2:3])
        for k in range(WIDE // CH):
            chi_ref[pl.ds(WIDE // CH * i + k, 1), :] = value[:, CH * k : CH * k + CH]
        return carry

    def net_short(i, carry):
        pre = layer(first_ref[96:192, 0:192], desc_ref[:, wide(i)])
        pre_ref[:, wide(i)] = by_type(i, pre[0:32], pre[32:64], pre[64:96])
        return carry

    def net_end(i, carry):
        rows = [charges_ref[pl.ds(WIDE // CH * i + k, 1), :] for k in range(WIDE // CH)]
        charge = jnp.concatenate(rows, axis=1)
        weight = by_type(i, tall_ref[0:32, 0:1], tall_ref[0:32, 1:2], tall_ref[0:32, 2:3])
        hidden = jnp.tanh(pre_ref[:, wide(i)] + weight * charge)
        value = layer(last_ref[16:32, 0:96], hidden)
        value = by_type(i, value[0:1], value[1:2], value[2:3])
        for k in range(WIDE // 128):
            row = pl.ds(WIDE // 128 * i + k, 1)
            out_short_ref[row, :] = value[:, 128 * k : 128 * k + 128]
            out_charges_ref[row, :] = charge[:, 128 * k : 128 * k + 128]
        return carry

    hardness = jnp.where(
        types_ref[...] == 0, hard_ref[0], jnp.where(types_ref[...] == 1, hard_ref[1], hard_ref[2])
    )
    for d in range(3):
        t = offs_ref[d]
        spline = [t, 1.0 - t]
        for order in (3, 4, 5):
            grown = []
            for k in range(order):
                term = None
                if k < order - 1:
                    term = (t + k) * spline[k]
                if k >= 1:
                    other = (order - k - t) * spline[k - 1]
                    term = other if term is None else term + other
                grown.append(term * (1.0 / (order - 1)))
            if order == 5:
                s_ref[d, 0] = -spline[3]
                s_ref[d, 1] = spline[3] - spline[2]
                s_ref[d, 2] = spline[2] - spline[1]
                s_ref[d, 3] = spline[1] - spline[0]
                s_ref[d, 4] = spline[0]
            spline = grown
        for j in range(5):
            w_ref[d, j] = spline[4 - j]

    for g in range(4):
        acc_ref[256 * g + 224 : 256 * g + 256, :] = jnp.zeros((32, 256), F32)

    def mask(table, d, c, count):
        base = base_ref[d, pl.ds(c, 1), :]
        place = lax.broadcasted_iota(jnp.int32, (count, CH), 0) - base
        result = jnp.zeros((count, CH), F32)
        for j in range(5):
            result = jnp.where(place == j, table[d, j, pl.ds(c, 1), :], result)
        return result

    def slope_masks(c, carry):
        high, low = split(mask(s_ref, 0, c, 64))
        sx_ref[c, 0:64, :], sx_ref[c, 64:128, :] = high, low
        sp_mask_ref[c], sq_mask_ref[c] = mask(s_ref, P_DIM, c, 32), mask(s_ref, Q_DIM, c, 32)
        return carry

    def build(c, a_ref, i, b_ref, values_ref, shift):
        m_x, m_p, m_q = mask(w_ref, 0, c, 64), mask(w_ref, P_DIM, c, 32), mask(w_ref, Q_DIM, c, 32)
        mx_ref[c], mp_ref[c], mq_ref[c] = m_x, m_p, m_q
        for q in range(28):
            high, low = split(m_p * m_q[q : q + 1, :])
            a_ref[i, 32 * q : 32 * q + 32, :] = high
            a_ref[i, 896 + 32 * q : 896 + 32 * q + 32, :] = low
        high, low = split(m_x)
        b_ref[128:192, :], b_ref[192:256, :] = high, low
        bx_ref[c, 0:64, :], bx_ref[c, 64:128, :] = high, low
        b_ref[0:64, :], b_ref[64:128, :] = split(m_x * (values_ref[pl.ds(c, 1), :] - shift))

    def gather_part(part, width):
        for g in range(4):
            acc_ref[256 * g : 256 * g + 224, 0:width] += (
                part[224 * g : 224 * g + 224] + part[896 + 224 * g : 896 + 224 * g + 224]
            )

    def spread_first(lo, hi):
        def step(i, carry):
            part = dot(a0_ref[i], b0_ref[...], ((1,), (1,)))
            build(2 * i + 1, a1_ref, i, b1_ref, chi_ref, shift)
            gather_part(part, 256)
            part = dot(a1_ref[i], b1_ref[...], ((1,), (1,)))
            after = lax.rem(i + 1, PAIRS)
            build(2 * after, a0_ref, after, b0_ref, chi_ref, shift)
            gather_part(part, 256)
            return carry

        lax.fori_loop(lo, hi, step, 0)

    def spread_image(lo, hi):
        def step(i, carry):
            for c, b_ref in ((2 * i, b0_ref), (2 * i + 1, b1_ref)):
                value = image_ref[pl.ds(c, 1), :] - shift2
                b_ref[0:64, :], b_ref[64:128, :] = split(mx_ref[c] * value)
            part = dot(a0_ref[i], b0_ref[0:128, :], ((1,), (1,)))
            other = dot(a1_ref[i], b1_ref[0:128, :], ((1,), (1,)))
            gather_part(part + other, 128)
            return carry

        lax.fori_loop(lo, hi, step, 0)

    def clear(width):
        for g in range(4):
            acc_ref[256 * g : 256 * g + 224, 0:width] = jnp.zeros((224, width), F32)

    lane = lax.broadcasted_iota(jnp.int32, (8, 128), 1)

    def pack(sums):
        tile = jnp.zeros((8, 128), F32)
        for k, value in enumerate(sums):
            tile = jnp.where(lane == k, value, tile)
        return tile

    def total(array):
        return jnp.sum(jnp.sum(array, axis=0, keepdims=True), axis=1, keepdims=True)

    def ar_start(phase, tile):
        peers, slots, me, base = ((to_p, arp_ref, ip, 112), (to_xq, arq_ref, mine, 120))[phase]
        slots[me] = tile
        ars_ref[phase] = tile
        return send_all(peers, lambda number: ars_ref.at[phase], slots.at[me], send, recv, base)

    def ar_done(phase, copies):
        wait_all(copies)
        return jnp.sum((arp_ref, arq_ref)[phase][...], axis=0)

    def prepare():
        row = lax.broadcasted_iota(jnp.int32, (M, LN), 0).astype(F32)
        f_q = signed(row)
        f_p = signed(lanes_ref[0:1, :] + (6 * mine).astype(F32))
        f_x = signed(lanes_ref[1:2, :] + (24 * ip).astype(F32))
        factor = 2.0 * math.pi / M
        wave = (factor * factor) * (f_q * f_q + (f_p * f_p + f_x * f_x))
        safe = jnp.where(wave > 0, wave, 1.0)
        green_ref[...] = jnp.where(
            wave > 0, (4.0 * math.pi / (M * M * M)) * jnp.exp((-0.5 * SMEAR * SMEAR) * wave) / safe, 0.0
        )
        for g in range(4):
            for h in range(2):
                r1b_ref[h, g, XR : XR + 8, :] = jnp.zeros((8, 128), F32)
        x2_ref[...] = jnp.zeros((256, LN), F32)
        r3x_ref[comb(7), :] = jnp.zeros((32, 128), F32)
        k3b_ref[192:256, :] = jnp.zeros((64, LN), F32)
        lax.fori_loop(0, ATOMS // WIDE, net_short, 0)

    def solve(local_sums=None, during=(), finish=None):
        halves_of = [slice(0, 128), slice(128, 256)]
        to_wait = []
        for h, lanes in enumerate(halves_of):
            r1_ref[h, ix] = sd_ref[ix, 0:XR, lanes]
            to_wait.append(
                send_all(to_x, lambda g: sd_ref.at[g, 0:XR, lanes], r1_ref.at[h, ix], send, recv, 4 * h)
            )
        if during:
            during[0]()
        moved = []
        for h in range(2):
            waits(to_wait[h])
            k1_ref[h] = dot3(hx_ref, r1_ref[h].reshape(4 * XR, 128)).reshape(8, 24, 128)
            r2_ref[h, ip] = k1_ref[h, ip]
            moved.append(
                send_all(to_p, lambda s: k1_ref.at[h, s], r2_ref.at[h, ip], send, recv, 8 + 8 * h)
            )
        if during:
            during[1]()
        to_wait += moved
        for h in range(2):
            waits(moved[h])
            for y in range(4 * h, min(4 * h + 4, 7)):
                for side in range(2):
                    x2_ref[32 * y : 32 * y + 24, 128 * side : 128 * side + 128] = lane_pick(
                        [(r2_ref[h, 4 * side + s], 32 * (s - y)) for s in range(4)], 32
                    )
        k2 = dot3((hp_ref[0, 0:M, :], hp_ref[1, 0:M, :]), x2_ref[...], ((1,), (1,)))
        lane = lax.broadcasted_iota(jnp.int32, (32, 128), 1)
        rest = jnp.zeros((32, 128), F32)
        for y in range(7):
            tile = k2[:, halves_of[y // 4]]
            start = 32 * (y % 4)
            m_ref[comb(y), :] = lane_pick(
                [(tile[32 * k : 32 * k + 32], 24 * k - start) for k in range(6)], 24
            )
            inside = (lane >= 16 * y) & (lane < 16 * y + 16)
            rest = jnp.where(inside, turn(tile[160:192], 120 - start + 16 * y), rest)
        m_ref[comb(7), :] = rest
        r3_ref[rows8(8 * mine), :] = m_ref[rows8(8 * mine), :]
        copies = send_all(
            to_xq, lambda n: m_ref.at[rows8(8 * n)], r3_ref.at[rows8(8 * mine)], send, recv, 24
        )
        to_wait.append(copies)
        waits(copies)
        rest = r3_ref[comb(7), :]
        for y in range(7):
            r3x_ref[comb(y), :] = jnp.where(lane < 16, turn(rest, -16 * y), 0.0)
        k3 = dot3(hq_ref, jnp.concatenate([r3_ref[...], r3x_ref[...]], axis=1))
        energy_density = k3 * k3 * green_ref[...]
        k3 = k3 * green_ref[...]
        z3 = dot3(hqt_ref, k3)
        z3_ref[...], z3x_ref[...] = z3[:, 0:128], z3[:, 128:256]
        rest = jnp.zeros((32, 128), F32)
        for y in range(7):
            inside = (lane >= 16 * y) & (lane < 16 * y + 16)
            rest = jnp.where(inside, turn(z3x_ref[comb(y), :], 16 * y), rest)
        z3_ref[comb(7), :] = rest
        r3b_ref[rows8(8 * mine), :] = z3_ref[rows8(8 * mine), :]
        copies = send_all(
            to_xq, lambda n: z3_ref.at[rows8(8 * n)], r3b_ref.at[rows8(8 * mine)], send, recv, 56
        )
        if local_sums is not None:
            sums = ar_start(0, pack(local_sums(total(energy_density))))
        to_wait.append(copies)
        waits(copies)
        if local_sums is not None:
            sums = ar_start(1, ar_done(0, sums))
        rest = r3b_ref[comb(7), :]
        loaded = [r3b_ref[comb(y), :] for y in range(7)]
        last = [jnp.where(lane >= 120, loaded[y], turn(rest, -16 * y)) for y in range(7)]
        for k in range(6):
            for h in range(2):
                k3b_ref[32 * k : 32 * k + 32, halves_of[h]] = lane_pick(
                    [
                        ((last if k == 5 else loaded)[y], 32 * (y % 4) - 24 * k)
                        for y in range(4 * h, min(4 * h + 4, 7))
                    ],
                    32,
                )
        turned = jnp.transpose(k3b_ref[...])
        high, low = split(turned)
        v2 = dot(high, hp_ref[0]) + (dot(low, hp_ref[0]) + dot(high, hp_ref[1]))
        moved = []
        for h in range(2):
            for s in range(8):
                lanes = halves_of[s // 4]
                m2b_ref[h, s] = lane_pick(
                    [(v2[32 * y : 32 * y + 24, lanes], 32 * (y - s)) for y in range(4 * h, min(4 * h + 4, 7))],
                    32,
                )
            r2b_ref[h, ip] = m2b_ref[h, ip]
            moved.append(
                send_all(to_p, lambda s: m2b_ref.at[h, s], r2b_ref.at[h, ip], send, recv, 88 + 8 * h)
            )
        to_wait += moved
        back = []
        for h in range(2):
            waits(moved[h])
            v1_ref[h] = dot3(hxt_ref, r2b_ref[h].reshape(M, 128)).reshape(4, XR, 128)
            r1b_ref[h, ix, 0:XR, :] = v1_ref[h, ix]
            back.append(
                send_all(to_x, lambda g: v1_ref.at[h, g], r1b_ref.at[h, ix, 0:XR], send, recv, 104 + 4 * h)
            )
        to_wait += back
        if finish is not None:
            finish(ar_done(1, sums))
        for copies in back:
            waits(copies)
        for copies in to_wait:
            for copy in copies:
                copy.wait_send()

    def field(g):
        return jnp.concatenate([r1b_ref[0, g], r1b_ref[1, g]], axis=1)

    def load_field(get):
        for g in range(4):
            high, low = split(get(g))
            both = jnp.concatenate([high.astype(F32), low.astype(F32)], axis=0)
            turned = jnp.transpose(both)[0:224, :].astype(BF16)
            phi_ref[224 * g : 224 * g + 224, 0:128] = turned
            phi_ref[224 * g : 224 * g + 224, 128:192] = turned[:, 0:64]

    def x_contract(table, c, slot):
        high, low = table[c, 0:64, :], table[c, 64:128, :]
        t_ref[slot] = dot(phi_ref[...], jnp.concatenate([high, high, low], axis=0))

    def fold(product):
        return (product[0:8] + product[8:16]) + (product[16:24] + product[24:32])

    def in_pairs(contract, reduce):
        contract(0, 0)

        def step(i, carry):
            contract(2 * i + 1, 1)
            reduce(2 * i, 0)
            contract(2 * lax.rem(i + 1, PAIRS), 0)
            reduce(2 * i + 1, 1)
            return carry

        lax.fori_loop(0, PAIRS, step, 0)

    def sample_image(values_ref):
        def reduce(c, slot):
            m_p = mp_ref[c]
            found = jnp.zeros((8, CH), F32)
            for q in range(28):
                found = found + fold(t_ref[slot, 32 * q : 32 * q + 32, :] * m_p) * mq_ref[c, q : q + 1, :]
            image_ref[pl.ds(c, 1), :] = jnp.sum(found, axis=0, keepdims=True)

        in_pairs(lambda c, slot: x_contract(bx_ref, c, slot), reduce)
        image_ref[...] = image_ref[...] + hardness * values_ref[...]

    def sample_forces():
        def contract(c, slot):
            x_contract(bx_ref, c, slot)
            x_contract(sx_ref, c, slot + 2)

        def reduce(c, slot):
            m_p, s_p = mp_ref[c], sp_mask_ref[c]
            along_x, along_p, along_q = (jnp.zeros((8, CH), F32) for _ in range(3))
            for q in range(28):
                block = t_ref[slot, 32 * q : 32 * q + 32, :]
                m_q = mq_ref[c, q : q + 1, :]
                along_q = along_q + fold(block * m_p) * sq_mask_ref[c, q : q + 1, :]
                along_p = along_p + fold(block * s_p) * m_q
                along_x = along_x + fold(t_ref[slot + 2, 32 * q : 32 * q + 32, :] * m_p) * m_q
            minus = -charges_ref[pl.ds(c, 1), :]
            for d, along in ((0, along_x), (P_DIM, along_p), (Q_DIM, along_q)):
                out_forces_ref[d : d + 1, part(c)] = minus * jnp.sum(along, axis=0, keepdims=True)

        in_pairs(contract, reduce)

    atoms = float(ATOMS * 256)
    clear(256)
    lax.fori_loop(0, ATOMS // WIDE, net_chi, 0)
    for copy in loads:
        copy.start()
    chi = chi_ref[...]
    local_sum = total(chi)
    shift = local_sum * (1.0 / ATOMS)
    build(0, a0_ref, 0, b0_ref, chi_ref, shift)
    spread_first(0, 2)
    pl.semaphore_wait(barrier, len(to_xq) + len(to_p))
    copies = ar_start(0, pack([local_sum]))
    spread_first(2, 4)
    copies = ar_start(1, ar_done(0, copies))
    spread_first(4, PAIRS)
    mean = ar_done(1, copies)[0:1, 0:1] * (1.0 / atoms)
    for g in range(4):
        turned = jnp.transpose(acc_ref[256 * g : 256 * g + 256, :])
        ones = turned[128:192] + turned[192:256]
        ones_ref[g] = ones
        density = (mean - shift) * ones - (turned[0:64] + turned[64:128])
        sp_ref[g] = density
        sd_ref[g] = density
    p0 = mean - chi
    p0_ref[...] = p0
    for copy in loads:
        copy.wait()
    solve(
        during=(
            prepare,
            lambda: lax.fori_loop(0, NCH, slope_masks, 0),
        )
    )
    for g in range(4):
        phi0_ref[g] = field(g)
    load_field(field)
    sample_image(p0_ref)

    image = image_ref[...]
    image_sum = total(image)
    shift2 = image_sum * (1.0 / ATOMS)
    sums = pack([total(p0 * p0), total(p0 * image), image_sum, total(image * image), total(p0)])
    clear(128)
    copies = ar_start(0, sums)
    spread_image(0, 3)
    copies = ar_start(1, ar_done(0, copies))
    spread_image(3, PAIRS)
    sums = ar_done(1, copies)
    norm0, curve0, image_total, image_square, p0_total = (sums[0:1, k : k + 1] for k in range(5))
    alpha0 = norm0 / curve0
    image_mean = image_total * (1.0 / atoms)
    norm1 = (
        norm0
        - 2.0 * alpha0 * (curve0 - image_mean * p0_total)
        + alpha0 * alpha0 * (image_square - image_mean * image_total)
    )
    beta = norm1 / norm0
    residual = p0 - alpha0 * (image - image_mean)
    d1_ref[...] = residual + beta * p0
    for g in range(4):
        turned = jnp.transpose(acc_ref[256 * g : 256 * g + 256, 0:128])
        sd_ref[g] = (
            (1.0 + beta) * sp_ref[g]
            + (alpha0 * (image_mean - shift2)) * ones_ref[g]
            - alpha0 * (turned[0:64] + turned[64:128])
        )
    d1 = d1_ref[...]
    def finish(sums):
        alpha1 = sums[0:1, 0:1] / sums[0:1, 1:2]
        charges_ref[...] = alpha0 * p0_ref[...] + alpha1 * d1_ref[...]
        for g in range(4):
            phi0_ref[g] = alpha0 * phi0_ref[g]
        alpha_ref[...] = jnp.zeros((8, 128), F32) + alpha1
        lax.fori_loop(0, ATOMS // WIDE, net_end, 0)

    solve(
        lambda energy: [total(residual * residual), total(hardness * d1 * d1) + energy],
        finish=finish,
    )
    alpha1 = alpha_ref[0:1, 0:1]
    load_field(lambda g: phi0_ref[g] + alpha1 * field(g))
    sample_forces()


def hand_over(*refs):
    for source, target in zip(refs[:3], refs[3:]):
        target[...] = source[...]


def per_device(
    descriptors, types, offsets, stencil_base, w_first, w_second, w_out, hardness,
    sr_first, sr_charge, sr_out,
):
    tabs = tables()
    vmem = pl.BlockSpec(memory_space=pltpu.VMEM)
    smem = pl.BlockSpec(memory_space=pltpu.SMEM)
    far = pl.BlockSpec(memory_space=pl.ANY)

    def held(*shape, dtype=F32):
        return pltpu.VMEM(shape, dtype)

    results = pl.pallas_call(
        kernel,
        out_shape=(
            jax.ShapeDtypeStruct((ATOMS // 128, 128), F32),
            jax.ShapeDtypeStruct((3, ATOMS), F32),
            jax.ShapeDtypeStruct((ATOMS // 128, 128), F32),
        ),
        in_specs=[far] + [vmem] * 3 + [smem] + [vmem] * 6 + [far] * 5 + [vmem],
        out_specs=(vmem, vmem, vmem),
        scratch_shapes=[
            held(3, 5, NCH, CH), held(3, 5, NCH, CH),
            held(NCH, 64, CH), held(NCH, 32, CH), held(NCH, 32, CH),
            held(NCH, 128, CH, dtype=BF16), held(NCH, 128, CH, dtype=BF16),
            held(NCH, 32, CH), held(NCH, 32, CH),
            held(PAIRS, 1792, CH, dtype=BF16), held(PAIRS, 1792, CH, dtype=BF16),
            held(256, CH, dtype=BF16), held(256, CH, dtype=BF16),
            held(1024, 256),
            held(4, 64, LN), held(4, 64, LN), held(4, 64, LN),
            held(2, 4, XR, 128), held(2, 8, 24, 128), held(2, 8, 24, 128),
            held(256, LN), held(256, 128), held(256, 128), held(256, 128), held(M, LN),
            held(256, 128), held(256, 128), held(256, 128), held(256, LN),
            held(2, 8, 24, 128), held(2, 8, 24, 128), held(2, 4, XR, 128),
            held(2, 4, 64, 128), held(4, 64, LN), held(896, 192, dtype=BF16),
            held(NCH, CH), held(NCH, CH), held(NCH, CH),
            held(4, 896, CH),
            held(8, 8, 128), held(32, 8, 128), held(2, 8, 128),
            held(NCH, CH, dtype=jnp.int32), held(3, NCH, CH), held(3, NCH, CH, dtype=jnp.int32),
            held(NCH, CH), held(NCH, CH), held(32, ATOMS),
            held(192, 128), held(96, 128), held(32, 128), held(128, 128),
            held(8, 128), held(192, 256, dtype=BF16), held(96, 128, dtype=BF16), held(32, 128, dtype=BF16),
            held(64, ATOMS), held(2, M, 224, dtype=BF16), held(2, 224, M, dtype=BF16),
            held(2, 256, 256, dtype=BF16), held(2, M, 256, dtype=BF16), held(2, 256, M, dtype=BF16),
            pltpu.SemaphoreType.DMA((9,)),
            pltpu.SemaphoreType.DMA((152,)),
            pltpu.SemaphoreType.DMA((152,)),
        ],
        compiler_params=pltpu.CompilerParams(
            collective_id=0, has_side_effects=True, vmem_limit_bytes=63 * 1024 * 1024
        ),
        name="equilibrate",
    )(
        descriptors, types.reshape(1, ATOMS), offsets, stencil_base, hardness,
        w_first, w_second, w_out, sr_first, sr_charge, sr_out,
        *[jnp.asarray(t) for t in tabs],
    )
    charges, forces, short_energy = pl.pallas_call(
        hand_over,
        out_shape=tuple(jax.ShapeDtypeStruct(r.shape, F32) for r in results),
        in_specs=[vmem] * 3,
        out_specs=(vmem,) * 3,
        name="hand_over",
    )(*results)
    return charges.reshape(ATOMS), forces, short_energy.reshape(ATOMS)


def solution(mesh):
    rows, columns = P(AXES), P(None, AXES)
    return jax.shard_map(
        per_device,
        mesh=mesh,
        in_specs=(columns, rows, columns, columns) + (P(),) * 7,
        out_specs=(rows, columns, rows),
        check_vma=False,
    )
```
